256 devices in a mesh: grp: 8 (over x_lo, y), tile: 32 (over z, x_hi, core).
Axes of the slice: x: 4 (x_hi: 2, x_lo: 2; x = x_hi * 2 + x_lo), y: 4, z: 8, core: 2. Of those that a mesh axis runs over, the one named last changes fastest.
Arguments:
- latents: bfloat16 [8, 4096, 1152], P('grp', 'tile'), may hold values from -6 to 6
- condition: bfloat16 [8, 1152], replicated, may hold values from -6 to 6
- w_modulate: bfloat16 [1152, 3456], P(None, 'grp'), may hold values from -1 to 1
- w_project: bfloat16 [1152, 3456], replicated, may hold values from -0.1875 to 0.1875
- w_output: bfloat16 [1152, 1152], replicated, may hold values from -0.1875 to 0.1875
- detail: int32 [8, 32], P('grp'), may hold values from 0 to 1, as said below
Outputs:
- updated: bfloat16 [8, 4096, 1152], P('grp', 'tile')
The draws below stay inside these ranges and needn't reach their ends.
Inputs may be any that keep to these rules, and one draw needn't show every extreme that they name: `detail`: at most 8 strips of an image are marked, and at least one.
All inputs are finite; a program needn't handle non-finite values.
Results may differ from the reference program's by a relative error of at most 0.012.
Values may be sent and summed in bfloat16 or wider, within the bound.
A program may use at most 192 MiB of HBM per device.

```python
import math
import jax
import jax.numpy as jnp
from jax import lax

D = 1152
HEADS = 16
HEAD = 72
ROW_TOKENS = 64
TOK_DEV = 128
TILES = 32
MARKED = 8
TOKENS = 4096
IMAGES = 8


def draw_w_modulate(key, part):
    base = jax.random.normal(key, (D, 3 * D), jnp.float32)
    values = jnp.clip(base, -6.0, 6.0) / math.sqrt(4.0 * D)
    return values.astype(jnp.bfloat16)


def draw_detail(key, part):
    count_key = jax.random.fold_in(key, 11)
    image_key = jax.random.fold_in(key, 23)
    order_key = jax.random.fold_in(key, 37)
    counts = jax.random.randint(count_key, (IMAGES,), 1, MARKED + 1)
    chosen = jax.random.randint(image_key, (), 0, IMAGES)
    counts = jnp.where(jnp.arange(IMAGES, dtype=jnp.int32) == chosen, MARKED, counts)
    image_keys = jax.random.split(order_key, IMAGES)

    def one_order(subkey):
        return jax.random.permutation(subkey, TILES)
    orders = jax.vmap(one_order)(image_keys)
    return (orders < counts[:, None]).astype(jnp.int32)


def level_of(stream_key, dims, cuts, low, top_value):
    gain, own = 1.0, jax.random.fold_in(stream_key, 6)
    for position, blocks in cuts:
        draws = jnp.exp(jax.random.uniform(jax.random.fold_in(own, position), (blocks,), jnp.float32, low / len(cuts), top_value / len(cuts)))
        gain = gain * jnp.repeat(draws, dims[position] // blocks).reshape([-1 if axis == position else 1 for axis in range(len(dims))])
    return gain


def bell_draw(own_key, shape, width, bound, pieces=(), held_as=jnp.bfloat16):
    values = width * jax.random.normal(own_key, shape, jnp.float32)
    if pieces:
        values = values * level_of(own_key, shape, pieces, -0.22, 0.18)
    return jnp.clip(values, -bound, bound).astype(held_as)


def setup_inputs(seed: int = 0) -> dict:
    key_of = jax.random.split(jax.random.key(seed), 7)
    latents = bell_draw(key_of[0], (IMAGES, TOKENS, D), 1.0, 6.0, ((0, 8), (1, 32)))
    condition = bell_draw(key_of[1], (IMAGES, D), 1.0, 6.0)
    w_modulate = draw_w_modulate(jax.random.fold_in(key_of[6], 71), 0)
    w_project = bell_draw(key_of[3], (D, 3 * D), D ** -0.5, 0.1875)
    w_output = bell_draw(key_of[4], (D, D), D ** -0.5, 0.1875)
    detail = draw_detail(jax.random.fold_in(key_of[6], 71), 0)
    return {"latents": latents, "condition": condition, "w_modulate": w_modulate, "w_project": w_project, "w_output": w_output, "detail": detail}


def attend(query, keys, values, valid):
    count = query.shape[0]
    heads_q = query.astype(jnp.float32).reshape(count, HEADS, HEAD)
    heads_k = keys.astype(jnp.float32).reshape(keys.shape[0], HEADS, HEAD)
    heads_v = values.astype(jnp.float32).reshape(values.shape[0], HEADS, HEAD)
    scores = jnp.einsum('qhd,khd->hqk', heads_q, heads_k) / jnp.sqrt(jnp.float32(HEAD))
    scores = jnp.where(valid[None, None, :], scores, jnp.float32(-1e+30))
    top = lax.optimization_barrier(jnp.max(scores, axis=2, keepdims=True))
    probs = jnp.exp(scores - top)
    total = lax.optimization_barrier(jnp.sum(probs, axis=2))
    weights = probs.astype(jnp.bfloat16).astype(jnp.float32)
    result = jnp.einsum('hqk,khd->qhd', weights, heads_v)
    return (result / jnp.transpose(total)[:, :, None]).reshape(count, D)

def reference(latents, condition, w_modulate, w_project, w_output, detail):
    modulation = jnp.dot(condition, w_modulate, preferred_element_type=jnp.float32)
    shift = modulation[:, :D]
    scale = modulation[:, D:2 * D]
    gate = modulation[:, 2 * D:]

    def one_image(packed):
        tokens, shift_row, scale_row, gate_row, marks = packed
        values32 = tokens.astype(jnp.float32)
        mean = lax.optimization_barrier(jnp.mean(values32, axis=1, keepdims=True))
        centered = values32 - mean
        variance = lax.optimization_barrier(jnp.mean(centered * centered, axis=1, keepdims=True))
        normed = (centered / jnp.sqrt(variance + 1e-06) * (1.0 + scale_row) + shift_row).astype(jnp.bfloat16)
        projected = jnp.dot(normed, w_project, preferred_element_type=jnp.float32).astype(jnp.bfloat16)
        query = projected[:, :D].reshape(TILES, TOK_DEV, D)
        pairs = projected[:, D:]
        strips = pairs.reshape(TILES, TOK_DEV, 2 * D)
        blank = jnp.zeros((1, ROW_TOKENS, 2 * D), jnp.bfloat16)
        before = jnp.concatenate([blank, strips[:-1, TOK_DEV - ROW_TOKENS:]], axis=0)
        after = jnp.concatenate([strips[1:, :ROW_TOKENS], blank], axis=0)
        extended = jnp.concatenate([before, strips, after], axis=1)
        tile_ids = jnp.arange(TILES, dtype=jnp.int32)
        lower = jnp.broadcast_to((tile_ids > 0)[:, None], (TILES, ROW_TOKENS))
        upper = jnp.broadcast_to((tile_ids < TILES - 1)[:, None], (TILES, ROW_TOKENS))
        inner = jnp.ones((TILES, TOK_DEV), dtype=bool)
        valid = jnp.concatenate([lower, inner, upper], axis=1)
        all_valid = jnp.ones((TOKENS,), dtype=bool)

        def strip_work(item):
            strip_q, strip_kv, strip_valid, mark = item
            near = attend(strip_q, strip_kv[:, :D], strip_kv[:, D:], strip_valid)
            whole = attend(strip_q, pairs[:, :D], pairs[:, D:], all_valid)
            return (near + mark.astype(jnp.float32) * whole).astype(jnp.bfloat16)
        mixed = lax.map(strip_work, (query, extended, valid, marks)).reshape(TOKENS, D)
        branch = jnp.dot(mixed, w_output, preferred_element_type=jnp.float32)
        return (values32 + gate_row * branch).astype(jnp.bfloat16)
    return lax.map(one_image, (latents, shift, scale, gate, detail))
```

```python
import functools

import jax
import jax.numpy as jnp
from jax import lax
from jax.experimental import pallas as pl
from jax.experimental.pallas import tpu as pltpu
from jax.sharding import PartitionSpec as P

HEADS = 16
HEAD = 72
D = HEADS * HEAD
STRIP = 128
MARGIN = 64
TILES = 32
SLOTS = 8
GROUPS = 8
COLS = 3 * D // GROUPS
SPAN = 640
ROWS = 224
PAD = 80
Q_AT = 2 * HEAD
V_AT = HEAD - 8
CHUNK = 4
EXP_SCALE = 1.4426950408889634 / (HEAD ** 0.5)
MESH = pl.DeviceIdType.MESH
F32 = jnp.float32
BF16 = jnp.bfloat16
ORDER = (8, 9, 6, 10, 7, 11, 12, 4, 13, 5, 2, 14, 3, 15, 1)


def body(
    x_hbm, cond_ref, wm_hbm, wp_hbm, wo_hbm, marks,
    out_ref,
    x_ref, wm, wp, wo, mod_send, mod_recv, mod, proj, send, buf, keys, q4, near, whole, osend, mixed,
    ranks,
    load_sem, mod_ssem, mod_rsem, send_sem, recv_sem, fwd_ssem, fwd_rsem, wh_sem, o_ssem, o_rsem,
):
    me = lax.axis_index("tile")
    grp = lax.axis_index("grp")
    chip = me // 2
    core = me % 2
    sibling = me + 1 - 2 * core

    barrier = pltpu.get_barrier_semaphore()
    for off in range(1, GROUPS):
        pl.semaphore_signal(barrier, inc=1, device_id={"grp": (grp + off) % GROUPS}, device_id_type=MESH)
    for off in range(1, HEADS):
        pl.semaphore_signal(
            barrier, inc=1, device_id={"tile": ((chip + off) % HEADS) * 2 + core}, device_id_type=MESH
        )
    pl.semaphore_signal(barrier, inc=1, device_id={"tile": sibling}, device_id_type=MESH)

    load_m = pltpu.make_async_copy(wm_hbm, wm, load_sem.at[0])
    load_x = pltpu.make_async_copy(x_hbm, x_ref, load_sem.at[1])
    load_p = [
        pltpu.make_async_copy(wp_hbm.at[:, pl.ds(D * i, D)], wp.at[i], load_sem.at[2 + i]) for i in range(3)
    ]
    load_o = pltpu.make_async_copy(wo_hbm, wo, load_sem.at[5])
    load_m.start()
    load_x.start()
    for copy in load_p:
        copy.start()
    load_o.start()

    load_m.wait()
    mod_send[...] = jnp.zeros_like(mod_send)
    mod_send[:, :COLS] = jnp.dot(cond_ref[...], wm[...], preferred_element_type=F32)
    mod_send[...] = pltpu.roll(mod_send[...], (grp * COLS) % 128, axis=1)

    load_x.wait()
    values32 = x_ref[...].astype(F32)
    mean = jnp.mean(values32, axis=1, keepdims=True)
    centered = values32 - mean
    variance = jnp.mean(centered * centered, axis=1, keepdims=True)
    unit = centered / jnp.sqrt(variance + 1e-06)

    rank = jnp.int32(0)
    slots = [jnp.int32(0)] * (SLOTS // 2)
    for t in range(TILES):
        mark = marks[0, t]
        for j in range(SLOTS // 2):
            hit = jnp.logical_and(mark > 0, rank == core * (SLOTS // 2) + j)
            slots[j] = jnp.where(hit, jnp.int32(t), slots[j])
        ranks[t] = jnp.minimum(rank, SLOTS - 1)
        rank = rank + mark

    pl.semaphore_wait(barrier, GROUPS - 1 + HEADS - 1 + 1)

    mod_copies = []
    for off in range(1, GROUPS):
        copy = pltpu.make_async_remote_copy(
            src_ref=mod_send, dst_ref=mod_recv.at[off - 1],
            send_sem=mod_ssem.at[off - 1], recv_sem=mod_rsem.at[off - 1],
            device_id={"grp": (grp + off) % GROUPS}, device_id_type=MESH,
        )
        copy.start()
        mod_copies.append(copy)
    mod[...] = jnp.zeros_like(mod)

    def add_columns(source, block):
        base = pl.multiple_of((source * COLS) // 128 * 128, 128)
        mod[:, pl.ds(base, SPAN)] += block

    add_columns(grp, mod_send[...])
    for off in range(1, GROUPS):
        mod_copies[off - 1].wait_recv()
        add_columns((grp + GROUPS - off) % GROUPS, mod_recv[off - 1])
    row = mod[pl.ds(grp, 1), :]
    shift = row[:, :D]
    scale = row[:, D : 2 * D]
    gate = row[:, 2 * D : 3 * D]
    normed = (unit * (1.0 + scale) + shift).astype(BF16)

    for part in range(3):
        load_p[part].wait()
        block = jnp.dot(normed, wp[part], preferred_element_type=F32)
        proj[part] = block.T
    for h in range(HEADS):
        rows = pl.ds(h * HEAD, HEAD)
        send[h] = jnp.concatenate(
            [proj[1, rows, :], proj[2, rows, :], proj[0, rows, :], jnp.zeros((8, STRIP), F32)], axis=0
        ).astype(BF16)

    copies = []
    for off in ORDER:
        other = (chip + off) % HEADS
        copy = pltpu.make_async_remote_copy(
            src_ref=send.at[other], dst_ref=buf.at[me],
            send_sem=send_sem.at[off], recv_sem=recv_sem.at[off],
            device_id={"tile": other * 2 + core}, device_id_type=MESH,
        )
        copy.start()
        copies.append(copy)

    def forward(off, src):
        strip = ((chip + HEADS - off) % HEADS) * 2 + core
        return pltpu.make_async_remote_copy(
            src_ref=src, dst_ref=buf.at[strip],
            send_sem=fwd_ssem.at[off], recv_sem=fwd_rsem.at[off],
            device_id={"tile": sibling}, device_id_type=MESH,
        )

    def store_keys(strip):
        block = buf[strip, 0:PAD, :].astype(F32).T
        keys[pl.ds(pl.multiple_of((strip + 1) * STRIP, STRIP), STRIP), :] = block.astype(BF16)

    keys[pl.ds(0, STRIP), :] = jnp.zeros((STRIP, PAD), BF16)
    keys[pl.ds((TILES + 1) * STRIP, STRIP), :] = jnp.zeros((STRIP, PAD), BF16)
    forwards = [forward(0, send.at[chip])]
    forwards[0].start()
    buf[me] = send[chip]
    store_keys(me)
    for off, copy in zip(ORDER, copies):
        copy.wait_recv()
        strip = ((chip + HEADS - off) % HEADS) * 2 + core
        passed = forward(off, buf.at[strip])
        passed.start()
        forwards.append(passed)
        store_keys(strip)
    for off, passed in zip((0,) + ORDER, forwards):
        passed.wait_recv()
        store_keys(((chip + HEADS - off) % HEADS) * 2 + 1 - core)

    for j in range(SLOTS // 2):
        q4[:, j * STRIP : (j + 1) * STRIP] = buf[slots[j], Q_AT:ROWS, :]
    wide = (SLOTS // 2) * STRIP

    def whole_step(i, state):
        top, total, acc = state
        span = CHUNK * STRIP
        block = keys[pl.ds(pl.multiple_of(STRIP + i * span, STRIP), span), :]
        scores = jnp.dot(block, q4[...], preferred_element_type=F32)
        merged = jnp.maximum(top, jnp.max(scores, axis=0, keepdims=True))
        factor = jnp.exp2((top - merged) * EXP_SCALE)
        probs = jnp.exp2((scores - merged) * EXP_SCALE)
        total = total * factor + jnp.sum(probs, axis=0, keepdims=True)
        values = jnp.concatenate([buf[i * CHUNK + j, V_AT : V_AT + PAD, :] for j in range(CHUNK)], axis=1)
        acc = acc * factor + jnp.dot(values, probs.astype(BF16), preferred_element_type=F32)
        return merged, total, acc

    state = (
        jnp.full((1, wide), -1e30, F32), jnp.zeros((1, wide), F32), jnp.zeros((PAD, wide), F32),
    )
    _, total, acc = lax.fori_loop(0, TILES // CHUNK, whole_step, state)
    result = acc / total
    for j in range(SLOTS // 2):
        whole[core * (SLOTS // 2) + j] = result[8:PAD, j * STRIP : (j + 1) * STRIP]
    mine = whole.at[pl.ds(core * (SLOTS // 2), SLOTS // 2)]
    swap = pltpu.make_async_remote_copy(
        src_ref=mine, dst_ref=mine, send_sem=wh_sem.at[0], recv_sem=wh_sem.at[1],
        device_id={"tile": sibling}, device_id_type=MESH,
    )
    swap.start()

    def near_step(j, carry):
        strip = 2 * j + core
        block = keys[pl.ds(pl.multiple_of((strip + 1) * STRIP - MARGIN, MARGIN), 2 * STRIP), :]
        scores = jnp.dot(block, buf[strip, Q_AT:ROWS, :], preferred_element_type=F32)
        at = strip * STRIP - MARGIN + lax.broadcasted_iota(jnp.int32, scores.shape, 0)
        scores = jnp.where(jnp.logical_and(at >= 0, at < TILES * STRIP), scores, -1e30)
        probs = jnp.exp2((scores - jnp.max(scores, axis=0, keepdims=True)) * EXP_SCALE)
        sums = jnp.sum(probs, axis=0, keepdims=True)
        blank = jnp.zeros((MARGIN, STRIP), BF16)
        weights = jnp.concatenate([blank, probs.astype(BF16), blank], axis=0)
        rows = pl.ds(V_AT, PAD)
        values = jnp.concatenate(
            [
                buf[jnp.maximum(strip - 1, 0), rows, :],
                buf[strip, rows, :],
                buf[jnp.minimum(strip + 1, TILES - 1), rows, :],
            ],
            axis=1,
        )
        near[j] = (jnp.dot(values, weights, preferred_element_type=F32) / sums)[8:PAD]
        return carry

    lax.fori_loop(0, TILES // 2, near_step, 0, unroll=4)
    swap.wait_recv()

    for j in range(TILES // 2):
        strip = 2 * j + core
        extra = whole[ranks[strip]]
        total = near[j] + jnp.where(marks[0, strip] > 0, extra, 0.0)
        osend[j] = jnp.concatenate([total, jnp.zeros((PAD - HEAD, STRIP), F32)], axis=0).astype(BF16)
    outs = []
    for off in ORDER:
        other = (chip + off) % HEADS
        copy = pltpu.make_async_remote_copy(
            src_ref=osend.at[other], dst_ref=mixed.at[chip],
            send_sem=o_ssem.at[off], recv_sem=o_rsem.at[off],
            device_id={"tile": other * 2 + core}, device_id_type=MESH,
        )
        copy.start()
        outs.append(copy)
    mixed[chip] = osend[chip]
    load_o.wait()
    for copy in outs:
        copy.wait_recv()

    gathered = jnp.concatenate([mixed[h, 0:HEAD, :].astype(F32) for h in range(HEADS)], axis=0).T
    branch = jnp.dot(gathered.astype(BF16), wo[...], preferred_element_type=F32)
    out_ref[...] = (x_ref[...].astype(F32) + gate * branch).astype(BF16)

    for copy in mod_copies + copies + forwards + outs + [swap]:
        copy.wait_send()


def on_device(latents, condition, w_modulate, w_project, w_output, detail):
    hbm = pl.BlockSpec(memory_space=pl.ANY)
    vmem = pl.BlockSpec(memory_space=pltpu.VMEM)
    dma = pltpu.SemaphoreType.DMA
    updated = pl.pallas_call(
        body,
        out_shape=jax.ShapeDtypeStruct((STRIP, D), BF16),
        in_specs=[hbm, vmem, hbm, hbm, hbm, pl.BlockSpec(memory_space=pltpu.SMEM)],
        out_specs=vmem,
        scratch_shapes=[
            pltpu.VMEM((STRIP, D), BF16),
            pltpu.VMEM((D, COLS), BF16),
            pltpu.VMEM((3, D, D), BF16),
            pltpu.VMEM((D, D), BF16),
            pltpu.VMEM((GROUPS, SPAN), F32),
            pltpu.VMEM((GROUPS - 1, GROUPS, SPAN), F32),
            pltpu.VMEM((GROUPS, 3 * D + 256), F32),
            pltpu.VMEM((3, D, STRIP), F32),
            pltpu.VMEM((HEADS, ROWS, STRIP), BF16),
            pltpu.VMEM((TILES, ROWS, STRIP), BF16),
            pltpu.VMEM(((TILES + 2) * STRIP, PAD), BF16),
            pltpu.VMEM((PAD, SLOTS // 2 * STRIP), BF16),
            pltpu.VMEM((TILES // 2, HEAD, STRIP), F32),
            pltpu.VMEM((SLOTS, HEAD, STRIP), F32),
            pltpu.VMEM((HEADS, PAD, STRIP), BF16),
            pltpu.VMEM((HEADS, PAD, STRIP), BF16),
            pltpu.SMEM((TILES,), jnp.int32),
            dma((6,)),
            dma((GROUPS - 1,)), dma((GROUPS - 1,)),
            dma((HEADS,)), dma((HEADS,)),
            dma((HEADS,)), dma((HEADS,)),
            dma((2,)),
            dma((HEADS,)), dma((HEADS,)),
        ],
        compiler_params=pltpu.CompilerParams(
            collective_id=0, has_side_effects=True, vmem_limit_bytes=56 * 1024 * 1024
        ),
    )(latents[0], condition, w_modulate, w_project, w_output, detail)
    return updated[None]


def solution(mesh):
    in_specs = (P("grp", "tile", None), P(), P(None, "grp"), P(), P(), P("grp", None))
    out_specs = P("grp", "tile", None)
    return jax.shard_map(
        on_device, mesh=mesh, in_specs=in_specs, out_specs=out_specs, check_vma=False
    )
```

```python
import functools

import jax
import jax.numpy as jnp
from jax import lax
from jax.experimental import pallas as pl
from jax.experimental.pallas import tpu as pltpu
from jax.sharding import PartitionSpec as P

HEADS = 16
HEAD = 72
D = HEADS * HEAD
STRIP = 128
MARGIN = 64
TILES = 32
SLOTS = 8
GROUPS = 8
COLS = 3 * D // GROUPS
SPAN = 640
PAD = 80
V_AT = HEAD - 8
SIDE = SLOTS // 2
WIDE = SIDE * STRIP
TILE_ROWS = 5
EXP_SCALE = 1.4426950408889634 / (HEAD ** 0.5)
MESH = pl.DeviceIdType.MESH
F32 = jnp.float32
BF16 = jnp.bfloat16
ORDER = (8, 9, 6, 10, 7, 11, 12, 4, 13, 5, 2, 14, 3, 15, 1)


def body(
    x_hbm, cond_hbm, wm_hbm, wp_hbm, wo_hbm, marks_hbm,
    out_ref,
    x_ref, cond, wm, wp, wo, mod_cols, mod_send, mod_recv, mod, proj, qsend, kvsend, qbuf, kvbuf, keys, q4,
    near, whole, osend, mixed, marks, ranks,
    load_sem, mod_ssem, mod_rsem, q_ssem, q_rsem, kv_ssem, kv_rsem, qf_ssem, qf_rsem, kvf_ssem, kvf_rsem,
    wh_sem, o_ssem, o_rsem,
):
    me = lax.axis_index("tile")
    grp = lax.axis_index("grp")
    chip = me // 2
    core = me % 2
    sibling = me + 1 - 2 * core

    barrier = pltpu.get_barrier_semaphore()
    for off in ORDER:
        pl.semaphore_signal(
            barrier, inc=1, device_id={"tile": ((chip + off) % HEADS) * 2 + core}, device_id_type=MESH
        )
    for off in range(1, GROUPS):
        pl.semaphore_signal(barrier, inc=1, device_id={"grp": (grp + off) % GROUPS}, device_id_type=MESH)
    pl.semaphore_signal(barrier, inc=1, device_id={"tile": sibling}, device_id_type=MESH)

    load_c = pltpu.make_async_copy(cond_hbm, cond, load_sem.at[6])
    load_m = pltpu.make_async_copy(wm_hbm, wm, load_sem.at[0])
    load_x = pltpu.make_async_copy(x_hbm, x_ref, load_sem.at[1])
    load_d = pltpu.make_async_copy(marks_hbm, marks, load_sem.at[7])
    load_p = [
        pltpu.make_async_copy(wp_hbm.at[:, pl.ds(D * i, D)], wp.at[i], load_sem.at[2 + i]) for i in range(3)
    ]
    load_o = pltpu.make_async_copy(wo_hbm, wo, load_sem.at[5])
    for copy in [load_c, load_m, load_x, load_d] + load_p + [load_o]:
        copy.start()

    mod_cols[...] = jnp.zeros_like(mod_cols)
    mod_send[...] = jnp.zeros_like(mod_send)
    mod[...] = jnp.zeros_like(mod)
    load_c.wait()
    load_m.wait()
    mod_cols[:, :COLS] = lax.dot_general(
        cond[...], wm[...], (((1,), (1,)), ((), ())), preferred_element_type=F32
    )
    shifted = pltpu.roll(mod_cols[...], (grp * COLS) % 128, axis=1)
    for i in range(TILE_ROWS):
        mod_send[:, i, :] = shifted[:, i * 128 : (i + 1) * 128]

    load_x.wait()
    values32 = x_ref[...].astype(F32)
    mean = jnp.mean(values32, axis=1, keepdims=True)
    centered = values32 - mean
    variance = jnp.mean(centered * centered, axis=1, keepdims=True)
    unit = centered / jnp.sqrt(variance + 1e-06)

    load_d.wait()
    rank = jnp.int32(0)
    slots = [jnp.int32(0)] * SIDE
    for t in range(TILES):
        mark = marks[0, t]
        for j in range(SIDE):
            hit = jnp.logical_and(mark > 0, rank == core * SIDE + j)
            slots[j] = jnp.where(hit, jnp.int32(t), slots[j])
        ranks[t] = jnp.minimum(rank, SLOTS - 1)
        rank = rank + mark

    pl.semaphore_wait(barrier, GROUPS - 1 + HEADS - 1 + 1)

    mod_copies = []
    for off in range(1, GROUPS):
        image = (grp + off) % GROUPS
        copy = pltpu.make_async_remote_copy(
            src_ref=mod_send.at[image], dst_ref=mod_recv.at[off - 1],
            send_sem=mod_ssem.at[off - 1], recv_sem=mod_rsem.at[off - 1],
            device_id={"grp": image}, device_id_type=MESH,
        )
        copy.start()
        mod_copies.append(copy)

    def add_columns(source, block):
        rows = pl.ds((source * COLS) // 128, TILE_ROWS)
        mod[rows, :] += block[0:TILE_ROWS]

    add_columns(grp, mod_send[grp])
    for off in range(1, GROUPS):
        mod_copies[off - 1].wait_recv()
        add_columns((grp + GROUPS - off) % GROUPS, mod_recv[off - 1])

    def mod_row(part):
        first = part * D // 128
        return jnp.concatenate([mod[first + i : first + i + 1, :] for i in range(D // 128)], axis=1)

    normed = (unit * (1.0 + mod_row(1)) + mod_row(0)).astype(BF16)

    def project(part):
        load_p[part].wait()
        proj[part] = jnp.dot(normed, wp[part], preferred_element_type=F32).T

    def exchange(src, dst, ssem, rsem):
        sent = []
        for off in ORDER:
            other = (chip + off) % HEADS
            copy = pltpu.make_async_remote_copy(
                src_ref=src.at[other], dst_ref=dst, send_sem=ssem.at[off], recv_sem=rsem.at[off],
                device_id={"tile": other * 2 + core}, device_id_type=MESH,
            )
            copy.start()
            sent.append(copy)
        return sent

    def forward(off, src, dst, ssem, rsem):
        copy = pltpu.make_async_remote_copy(
            src_ref=src, dst_ref=dst.at[strip_of(off, core)], send_sem=ssem.at[off], recv_sem=rsem.at[off],
            device_id={"tile": sibling}, device_id_type=MESH,
        )
        copy.start()
        return copy

    def strip_of(off, parity):
        return ((chip + HEADS - off) % HEADS) * 2 + parity

    project(0)
    for h in range(HEADS):
        qsend[h] = jnp.concatenate(
            [proj[0, h * HEAD : (h + 1) * HEAD, :], jnp.zeros((PAD - HEAD, STRIP), F32)], axis=0
        ).astype(BF16)
    q_sent = exchange(qsend, qbuf.at[me], q_ssem, q_rsem)
    q_passed = [forward(0, qsend.at[chip], qbuf, qf_ssem, qf_rsem)]
    qbuf[me] = qsend[chip]
    project(1)
    project(2)
    for h in range(HEADS):
        rows = slice(h * HEAD, (h + 1) * HEAD)
        kvsend[h] = jnp.concatenate([proj[1, rows, :], proj[2, rows, :]], axis=0).astype(BF16)
    kv_sent = exchange(kvsend, kvbuf.at[me], kv_ssem, kv_rsem)
    kv_passed = [forward(0, kvsend.at[chip], kvbuf, kvf_ssem, kvf_rsem)]
    kvbuf[me] = kvsend[chip]
    keys[pl.ds(0, STRIP), :] = jnp.zeros((STRIP, PAD), BF16)
    keys[pl.ds((TILES + 1) * STRIP, STRIP), :] = jnp.zeros((STRIP, PAD), BF16)

    for off, copy in zip(ORDER, q_sent):
        copy.wait_recv()
        q_passed.append(forward(off, qbuf.at[strip_of(off, core)], qbuf, qf_ssem, qf_rsem))
    for copy in q_passed:
        copy.wait_recv()
    for j in range(SIDE):
        q4[:, j * STRIP : (j + 1) * STRIP] = qbuf[slots[j]]

    def whole_step(off, state):
        top, total, acc = state
        pair = (chip + HEADS - off) % HEADS
        for parity in range(2):
            strip = pair * 2 + parity
            block = kvbuf[strip, 0:PAD, :].astype(F32).T
            keys[pl.ds(pl.multiple_of((strip + 1) * STRIP, STRIP), STRIP), :] = block.astype(BF16)
        block = keys[pl.ds(pl.multiple_of((2 * pair + 1) * STRIP, STRIP), 2 * STRIP), :]
        scores = jnp.dot(block, q4[...], preferred_element_type=F32)
        merged = jnp.maximum(top, jnp.max(scores, axis=0, keepdims=True))
        factor = jnp.exp2((top - merged) * EXP_SCALE)
        probs = jnp.exp2((scores - merged) * EXP_SCALE)
        total = total * factor + jnp.sum(probs, axis=0, keepdims=True)
        rows = slice(V_AT, V_AT + PAD)
        values = jnp.concatenate([kvbuf[2 * pair, rows, :], kvbuf[2 * pair + 1, rows, :]], axis=1)
        acc = acc * factor + jnp.dot(values, probs.astype(BF16), preferred_element_type=F32)
        return merged, total, acc

    state = (
        jnp.full((1, WIDE), -1e30, F32), jnp.zeros((1, WIDE), F32), jnp.zeros((PAD, WIDE), F32),
    )
    steps = (0,) + ORDER
    for i, off in enumerate(steps):
        if i + 1 < len(steps):
            kv_sent[i].wait_recv()
            later = steps[i + 1]
            kv_passed.append(forward(later, kvbuf.at[strip_of(later, core)], kvbuf, kvf_ssem, kvf_rsem))
        kv_passed[i].wait_recv()
        state = whole_step(off, state)
    _, total, acc = state
    result = acc / total
    for j in range(SIDE):
        whole[core * SIDE + j] = result[8:PAD, j * STRIP : (j + 1) * STRIP]
    mine = whole.at[pl.ds(core * SIDE, SIDE)]
    swap = pltpu.make_async_remote_copy(
        src_ref=mine, dst_ref=mine, send_sem=wh_sem.at[0], recv_sem=wh_sem.at[1],
        device_id={"tile": sibling}, device_id_type=MESH,
    )
    swap.start()

    def near_step(j, carry):
        strip = 2 * j + core
        block = keys[pl.ds(pl.multiple_of((strip + 1) * STRIP - MARGIN, MARGIN), 2 * STRIP), :]
        scores = jnp.dot(block, qbuf[strip], preferred_element_type=F32)
        at = strip * STRIP - MARGIN + lax.broadcasted_iota(jnp.int32, scores.shape, 0)
        scores = jnp.where(jnp.logical_and(at >= 0, at < TILES * STRIP), scores, -1e30)
        probs = jnp.exp2((scores - jnp.max(scores, axis=0, keepdims=True)) * EXP_SCALE)
        sums = jnp.sum(probs, axis=0, keepdims=True)
        blank = jnp.zeros((MARGIN, STRIP), BF16)
        weights = jnp.concatenate([blank, probs.astype(BF16), blank], axis=0)
        rows = pl.ds(V_AT, PAD)
        values = jnp.concatenate(
            [
                kvbuf[jnp.maximum(strip - 1, 0), rows, :],
                kvbuf[strip, rows, :],
                kvbuf[jnp.minimum(strip + 1, TILES - 1), rows, :],
            ],
            axis=1,
        )
        near[j] = (jnp.dot(values, weights, preferred_element_type=F32) / sums)[8:PAD]
        return carry

    lax.fori_loop(0, TILES // 2, near_step, 0, unroll=4)
    swap.wait_recv()

    for j in range(TILES // 2):
        strip = 2 * j + core
        extra = whole[ranks[strip]]
        total = near[j] + jnp.where(marks[0, strip] > 0, extra, 0.0)
        osend[j] = jnp.concatenate(
            [total[8 * r : 8 * r + 8] for r in range(HEAD // 8)], axis=1
        ).astype(BF16)
    outs = exchange(osend, mixed.at[chip], o_ssem, o_rsem)
    mixed[chip] = osend[chip]
    load_o.wait()
    for copy in outs:
        copy.wait_recv()

    gathered = []
    for h in range(HEADS):
        block = mixed[h].astype(F32)
        gathered += [block[:, 128 * r : 128 * r + 128] for r in range(HEAD // 8)]
    gathered = jnp.concatenate(gathered, axis=0).T
    branch = jnp.dot(gathered.astype(BF16), wo[...], preferred_element_type=F32)
    out_ref[...] = (x_ref[...].astype(F32) + mod_row(2) * branch).astype(BF16)

    for copy in mod_copies + q_sent + q_passed + kv_sent + kv_passed + outs + [swap]:
        copy.wait_send()


def on_device(latents, condition, w_modulate, w_project, w_output, detail):
    hbm = pl.BlockSpec(memory_space=pl.ANY)
    dma = pltpu.SemaphoreType.DMA
    updated = pl.pallas_call(
        body,
        out_shape=jax.ShapeDtypeStruct((STRIP, D), BF16),
        in_specs=[hbm] * 6,
        out_specs=pl.BlockSpec(memory_space=pltpu.VMEM),
        scratch_shapes=[
            pltpu.VMEM((STRIP, D), BF16),
            pltpu.VMEM((GROUPS, D), BF16),
            pltpu.VMEM((COLS, D), BF16),
            pltpu.VMEM((3, D, D), BF16),
            pltpu.VMEM((D, D), BF16),
            pltpu.VMEM((GROUPS, SPAN), F32),
            pltpu.VMEM((GROUPS, 8, 128), F32),
            pltpu.VMEM((GROUPS - 1, 8, 128), F32),
            pltpu.VMEM((32, 128), F32),
            pltpu.VMEM((3, D, STRIP), F32),
            pltpu.VMEM((HEADS, PAD, STRIP), BF16),
            pltpu.VMEM((HEADS, 2 * HEAD, STRIP), BF16),
            pltpu.VMEM((TILES, PAD, STRIP), BF16),
            pltpu.VMEM((TILES, 2 * HEAD, STRIP), BF16),
            pltpu.VMEM(((TILES + 2) * STRIP, PAD), BF16),
            pltpu.VMEM((PAD, WIDE), BF16),
            pltpu.VMEM((TILES // 2, HEAD, STRIP), F32),
            pltpu.VMEM((SLOTS, HEAD, STRIP), F32),
            pltpu.VMEM((HEADS, 8, D), BF16),
            pltpu.VMEM((HEADS, 8, D), BF16),
            pltpu.SMEM((1, TILES), jnp.int32),
            pltpu.SMEM((TILES,), jnp.int32),
            dma((8,)),
            dma((GROUPS - 1,)), dma((GROUPS - 1,)),
            dma((HEADS,)), dma((HEADS,)),
            dma((HEADS,)), dma((HEADS,)),
            dma((HEADS,)), dma((HEADS,)),
            dma((HEADS,)), dma((HEADS,)),
            dma((2,)),
            dma((HEADS,)), dma((HEADS,)),
        ],
        compiler_params=pltpu.CompilerParams(
            collective_id=0, has_side_effects=True, vmem_limit_bytes=56 * 1024 * 1024
        ),
    )(latents[0], condition, w_modulate.T, w_project, w_output, detail)
    return updated[None]


def solution(mesh):
    in_specs = (P("grp", "tile", None), P(), P(None, "grp"), P(), P(), P("grp", None))
    out_specs = P("grp", "tile", None)
    return jax.shard_map(
        on_device, mesh=mesh, in_specs=in_specs, out_specs=out_specs, check_vma=False
    )
```

```python
import functools

import jax
import jax.numpy as jnp
from jax import lax
from jax.experimental import pallas as pl
from jax.experimental.pallas import tpu as pltpu
from jax.sharding import PartitionSpec as P

HEADS = 16
HEAD = 72
D = HEADS * HEAD
STRIP = 128
MARGIN = 64
TILES = 32
SLOTS = 8
GROUPS = 8
COLS = 3 * D // GROUPS
SPAN = 640
PAD = 80
V_AT = HEAD - 8
SIDE = SLOTS // 2
WIDE = SIDE * STRIP
TILE_ROWS = 5
EXP_SCALE = 1.4426950408889634 / (HEAD ** 0.5)
MESH = pl.DeviceIdType.MESH
F32 = jnp.float32
BF16 = jnp.bfloat16
ORDER = (8, 9, 6, 10, 7, 11, 12, 4, 13, 5, 2, 14, 3, 15, 1)


def body(
    x_hbm, cond_hbm, wm_hbm, wp_hbm, wo_hbm, marks_hbm,
    out_ref,
    x_ref, cond, wm, wp, wo, mod_cols, mod_send, mod_recv, mod, proj, qsend, kvsend, qbuf, kvbuf, keys, q4,
    score_buf, near, whole, osend, mixed, marks, ranks,
    load_sem, mod_ssem, mod_rsem, q_ssem, q_rsem, kv_ssem, kv_rsem, qf_ssem, qf_rsem, kvf_ssem, kvf_rsem,
    wh_sem, o_ssem, o_rsem,
):
    me = lax.axis_index("tile")
    grp = lax.axis_index("grp")
    chip = me // 2
    core = me % 2
    sibling = me + 1 - 2 * core

    barrier = pltpu.get_barrier_semaphore()
    for off in ORDER:
        pl.semaphore_signal(
            barrier, inc=1, device_id={"tile": ((chip + off) % HEADS) * 2 + core}, device_id_type=MESH
        )
    for off in range(1, GROUPS):
        pl.semaphore_signal(barrier, inc=1, device_id={"grp": (grp + off) % GROUPS}, device_id_type=MESH)
    pl.semaphore_signal(barrier, inc=1, device_id={"tile": sibling}, device_id_type=MESH)

    load_c = pltpu.make_async_copy(cond_hbm, cond, load_sem.at[6])
    load_m = pltpu.make_async_copy(wm_hbm, wm, load_sem.at[0])
    load_x = pltpu.make_async_copy(x_hbm, x_ref, load_sem.at[1])
    load_d = pltpu.make_async_copy(marks_hbm, marks, load_sem.at[7])
    load_p = [
        pltpu.make_async_copy(wp_hbm.at[:, pl.ds(D * i, D)], wp.at[i], load_sem.at[2 + i]) for i in range(3)
    ]
    load_o = pltpu.make_async_copy(wo_hbm, wo, load_sem.at[5])
    for copy in (load_c, load_m, load_x, load_d):
        copy.start()

    mod_cols[...] = jnp.zeros_like(mod_cols)
    mod_send[...] = jnp.zeros_like(mod_send)
    mod[...] = jnp.zeros_like(mod)
    load_c.wait()
    load_m.wait()
    for copy in load_p + [load_o]:
        copy.start()
    mod_cols[:, :COLS] = lax.dot_general(
        cond[...], wm[...], (((1,), (1,)), ((), ())), preferred_element_type=F32
    )
    shifted = pltpu.roll(mod_cols[...], (grp * COLS) % 128, axis=1)
    for i in range(TILE_ROWS):
        mod_send[:, i, :] = shifted[:, i * 128 : (i + 1) * 128]

    pl.semaphore_wait(barrier, GROUPS - 1 + HEADS - 1 + 1)

    mod_copies = []
    for off in range(1, GROUPS):
        image = (grp + off) % GROUPS
        copy = pltpu.make_async_remote_copy(
            src_ref=mod_send.at[image], dst_ref=mod_recv.at[off - 1],
            send_sem=mod_ssem.at[off - 1], recv_sem=mod_rsem.at[off - 1],
            device_id={"grp": image}, device_id_type=MESH,
        )
        copy.start()
        mod_copies.append(copy)

    load_x.wait()
    values32 = x_ref[...].astype(F32)
    mean = jnp.mean(values32, axis=1, keepdims=True)
    centered = values32 - mean
    variance = jnp.mean(centered * centered, axis=1, keepdims=True)
    unit = centered / jnp.sqrt(variance + 1e-06)

    load_d.wait()
    rank = jnp.int32(0)
    slots = [jnp.int32(0)] * SIDE
    for t in range(TILES):
        mark = marks[0, t]
        for j in range(SIDE):
            hit = jnp.logical_and(mark > 0, rank == core * SIDE + j)
            slots[j] = jnp.where(hit, jnp.int32(t), slots[j])
        ranks[t] = jnp.minimum(rank, SLOTS - 1)
        rank = rank + mark

    def add_columns(source, block):
        rows = pl.ds((source * COLS) // 128, TILE_ROWS)
        mod[rows, :] += block[0:TILE_ROWS]

    add_columns(grp, mod_send[grp])
    for off in range(1, GROUPS):
        mod_copies[off - 1].wait_recv()
        add_columns((grp + GROUPS - off) % GROUPS, mod_recv[off - 1])

    def mod_row(part):
        first = part * D // 128
        return jnp.concatenate([mod[first + i : first + i + 1, :] for i in range(D // 128)], axis=1)

    normed = (unit * (1.0 + mod_row(1)) + mod_row(0)).astype(BF16)

    def project(part):
        load_p[part].wait()
        proj[part] = jnp.dot(normed, wp[part], preferred_element_type=F32).T

    def exchange(off, src, dst, ssem, rsem):
        other = (chip + off) % HEADS
        copy = pltpu.make_async_remote_copy(
            src_ref=src.at[other], dst_ref=dst, send_sem=ssem.at[off], recv_sem=rsem.at[off],
            device_id={"tile": other * 2 + core}, device_id_type=MESH,
        )
        copy.start()
        return copy

    def forward(off, src, dst, ssem, rsem):
        copy = pltpu.make_async_remote_copy(
            src_ref=src, dst_ref=dst.at[strip_of(off, core)], send_sem=ssem.at[off], recv_sem=rsem.at[off],
            device_id={"tile": sibling}, device_id_type=MESH,
        )
        copy.start()
        return copy

    def strip_of(off, parity):
        return ((chip + HEADS - off) % HEADS) * 2 + parity

    project(0)
    for h in range(HEADS):
        qsend[h] = jnp.concatenate(
            [proj[0, h * HEAD : (h + 1) * HEAD, :], jnp.zeros((PAD - HEAD, STRIP), F32)], axis=0
        ).astype(BF16)
    q_sent = [exchange(off, qsend, qbuf.at[me], q_ssem, q_rsem) for off in ORDER]
    q_passed = [forward(0, qsend.at[chip], qbuf, qf_ssem, qf_rsem)]
    qbuf[me] = qsend[chip]
    project(1)
    project(2)
    for h in range(HEADS):
        rows = slice(h * HEAD, (h + 1) * HEAD)
        kvsend[h] = jnp.concatenate([proj[1, rows, :], proj[2, rows, :]], axis=0).astype(BF16)
    kv_sent = []
    kv_passed = [forward(0, kvsend.at[chip], kvbuf, kvf_ssem, kvf_rsem)]
    kvbuf[me] = kvsend[chip]
    keys[pl.ds(0, STRIP), :] = jnp.zeros((STRIP, PAD), BF16)
    keys[pl.ds((TILES + 1) * STRIP, STRIP), :] = jnp.zeros((STRIP, PAD), BF16)

    for off, copy in zip(ORDER, q_sent):
        copy.wait_send()
        kv_sent.append(exchange(off, kvsend, kvbuf.at[me], kv_ssem, kv_rsem))
    for off, copy in zip(ORDER, q_sent):
        copy.wait_recv()
        q_passed.append(forward(off, qbuf.at[strip_of(off, core)], qbuf, qf_ssem, qf_rsem))
    for copy in q_passed:
        copy.wait_recv()
    for j in range(SIDE):
        q4[:, j * STRIP : (j + 1) * STRIP] = qbuf[slots[j]]

    def pair_of(off):
        return (chip + HEADS - off) % HEADS

    def scores_step(i, off, top):
        pair = pair_of(off)
        for parity in range(2):
            strip = pair * 2 + parity
            block = kvbuf[strip, 0:PAD, :].astype(F32).T
            keys[pl.ds(pl.multiple_of((strip + 1) * STRIP, STRIP), STRIP), :] = block.astype(BF16)
        block = keys[pl.ds(pl.multiple_of((2 * pair + 1) * STRIP, STRIP), 2 * STRIP), :]
        scores = jnp.dot(block, q4[...], preferred_element_type=F32)
        score_buf[i % 2] = scores
        return jnp.maximum(top, jnp.max(scores, axis=0, keepdims=True))

    def values_step(i, off, before, top, total, acc):
        pair = pair_of(off)
        factor = jnp.exp2((before - top) * EXP_SCALE)
        probs = jnp.exp2((score_buf[i % 2] - top) * EXP_SCALE)
        total = total * factor + jnp.sum(probs, axis=0, keepdims=True)
        rows = slice(V_AT, V_AT + PAD)
        values = jnp.concatenate([kvbuf[2 * pair, rows, :], kvbuf[2 * pair + 1, rows, :]], axis=1)
        acc = acc * factor + jnp.dot(values, probs.astype(BF16), preferred_element_type=F32)
        return total, acc

    def near_step(off):
        pair = pair_of(off)
        strip = 2 * pair + core
        block = keys[pl.ds(pl.multiple_of((strip + 1) * STRIP - MARGIN, MARGIN), 2 * STRIP), :]
        scores = jnp.dot(block, qbuf[strip], preferred_element_type=F32)
        at = strip * STRIP - MARGIN + lax.broadcasted_iota(jnp.int32, scores.shape, 0)
        scores = jnp.where(jnp.logical_and(at >= 0, at < TILES * STRIP), scores, -1e30)
        probs = jnp.exp2((scores - jnp.max(scores, axis=0, keepdims=True)) * EXP_SCALE)
        sums = jnp.sum(probs, axis=0, keepdims=True)
        blank = jnp.zeros((MARGIN, STRIP), BF16)
        weights = jnp.concatenate([blank, probs.astype(BF16), blank], axis=0)
        rows = pl.ds(V_AT, PAD)
        values = jnp.concatenate(
            [
                kvbuf[jnp.maximum(strip - 1, 0), rows, :],
                kvbuf[strip, rows, :],
                kvbuf[jnp.minimum(strip + 1, TILES - 1), rows, :],
            ],
            axis=1,
        )
        near[pair] = (jnp.dot(values, weights, preferred_element_type=F32) / sums)[8:PAD]

    steps = (0,) + ORDER
    total = jnp.zeros((1, WIDE), F32)
    acc = jnp.zeros((PAD, WIDE), F32)
    tops = [jnp.full((1, WIDE), -1e30, F32)]
    ready = []
    done = 0
    for i, off in enumerate(steps):
        if i + 1 < len(steps):
            kv_sent[i].wait_recv()
            later = steps[i + 1]
            kv_passed.append(forward(later, kvbuf.at[strip_of(later, core)], kvbuf, kvf_ssem, kvf_rsem))
        kv_passed[i].wait_recv()
        tops.append(scores_step(i, off, tops[i]))
        if i > 0:
            total, acc = values_step(i - 1, steps[i - 1], tops[i - 1], tops[i], total, acc)
            for strip_off in ready[done:]:
                near_step(strip_off)
            done = len(ready)
        come = steps[: i + 1]
        for o in come:
            if o not in ready and (o + 1) % HEADS in come and (o - 1) % HEADS in come:
                ready.append(o)
    last = len(steps) - 1
    total, acc = values_step(last, steps[last], tops[last], tops[last + 1], total, acc)
    result = acc / total
    for j in range(SIDE):
        whole[core * SIDE + j] = result[8:PAD, j * STRIP : (j + 1) * STRIP]
    mine = whole.at[pl.ds(core * SIDE, SIDE)]
    swap = pltpu.make_async_remote_copy(
        src_ref=mine, dst_ref=mine, send_sem=wh_sem.at[0], recv_sem=wh_sem.at[1],
        device_id={"tile": sibling}, device_id_type=MESH,
    )
    swap.start()
    for strip_off in ready[done:]:
        near_step(strip_off)
    swap.wait_recv()

    for j in range(TILES // 2):
        strip = 2 * j + core
        extra = whole[ranks[strip]]
        total = near[j] + jnp.where(marks[0, strip] > 0, extra, 0.0)
        osend[j] = jnp.concatenate(
            [total[8 * r : 8 * r + 8] for r in range(HEAD // 8)], axis=1
        ).astype(BF16)
    outs = [exchange(off, osend, mixed.at[chip], o_ssem, o_rsem) for off in ORDER]
    mixed[chip] = osend[chip]
    load_o.wait()
    for copy in outs:
        copy.wait_recv()

    gathered = []
    for h in range(HEADS):
        block = mixed[h].astype(F32)
        gathered += [block[:, 128 * r : 128 * r + 128] for r in range(HEAD // 8)]
    gathered = jnp.concatenate(gathered, axis=0).T
    branch = jnp.dot(gathered.astype(BF16), wo[...], preferred_element_type=F32)
    out_ref[...] = (x_ref[...].astype(F32) + mod_row(2) * branch).astype(BF16)

    for copy in mod_copies + q_passed + kv_sent + kv_passed + outs + [swap]:
        copy.wait_send()


def on_device(latents, condition, w_modulate, w_project, w_output, detail):
    hbm = pl.BlockSpec(memory_space=pl.ANY)
    dma = pltpu.SemaphoreType.DMA
    updated = pl.pallas_call(
        body,
        out_shape=jax.ShapeDtypeStruct((STRIP, D), BF16),
        in_specs=[hbm] * 6,
        out_specs=pl.BlockSpec(memory_space=pltpu.VMEM),
        scratch_shapes=[
            pltpu.VMEM((STRIP, D), BF16),
            pltpu.VMEM((GROUPS, D), BF16),
            pltpu.VMEM((COLS, D), BF16),
            pltpu.VMEM((3, D, D), BF16),
            pltpu.VMEM((D, D), BF16),
            pltpu.VMEM((GROUPS, SPAN), F32),
            pltpu.VMEM((GROUPS, 8, 128), F32),
            pltpu.VMEM((GROUPS - 1, 8, 128), F32),
            pltpu.VMEM((32, 128), F32),
            pltpu.VMEM((3, D, STRIP), F32),
            pltpu.VMEM((HEADS, PAD, STRIP), BF16),
            pltpu.VMEM((HEADS, 2 * HEAD, STRIP), BF16),
            pltpu.VMEM((TILES, PAD, STRIP), BF16),
            pltpu.VMEM((TILES, 2 * HEAD, STRIP), BF16),
            pltpu.VMEM(((TILES + 2) * STRIP, PAD), BF16),
            pltpu.VMEM((PAD, WIDE), BF16),
            pltpu.VMEM((2, 2 * STRIP, WIDE), F32),
            pltpu.VMEM((TILES // 2, HEAD, STRIP), F32),
            pltpu.VMEM((SLOTS, HEAD, STRIP), F32),
            pltpu.VMEM((HEADS, 8, D), BF16),
            pltpu.VMEM((HEADS, 8, D), BF16),
            pltpu.SMEM((1, TILES), jnp.int32),
            pltpu.SMEM((TILES,), jnp.int32),
            dma((8,)),
            dma((GROUPS - 1,)), dma((GROUPS - 1,)),
            dma((HEADS,)), dma((HEADS,)),
            dma((HEADS,)), dma((HEADS,)),
            dma((HEADS,)), dma((HEADS,)),
            dma((HEADS,)), dma((HEADS,)),
            dma((2,)),
            dma((HEADS,)), dma((HEADS,)),
        ],
        compiler_params=pltpu.CompilerParams(
            collective_id=0, has_side_effects=True, vmem_limit_bytes=56 * 1024 * 1024
        ),
    )(latents[0], condition, w_modulate.T, w_project, w_output, detail)
    return updated[None]


def solution(mesh):
    in_specs = (P("grp", "tile", None), P(), P(None, "grp"), P(), P(), P("grp", None))
    out_specs = P("grp", "tile", None)
    return jax.shard_map(
        on_device, mesh=mesh, in_specs=in_specs, out_specs=out_specs, check_vma=False
    )
```

```python
import functools

import jax
import jax.numpy as jnp
from jax import lax
from jax.experimental import pallas as pl
from jax.experimental.pallas import tpu as pltpu
from jax.sharding import PartitionSpec as P

HEADS = 16
HEAD = 72
D = HEADS * HEAD
STRIP = 128
MARGIN = 64
TILES = 32
SLOTS = 8
GROUPS = 8
COLS = 3 * D // GROUPS
SPAN = 640
PAD = 80
V_AT = HEAD - 8
SIDE = SLOTS // 2
WIDE = SIDE * STRIP
TILE_ROWS = 5
AHEAD = 2
EXP_SCALE = 1.4426950408889634 / (HEAD ** 0.5)
MESH = pl.DeviceIdType.MESH
F32 = jnp.float32
BF16 = jnp.bfloat16
ORDER = (8, 9, 6, 10, 7, 11, 12, 4, 13, 5, 2, 14, 3, 15, 1)


def body(
    x_hbm, cond_hbm, wm_hbm, wp_hbm, wo_hbm, marks_hbm,
    out_ref,
    x_ref, cond, wm, wp, wo, mod_cols, mod_send, mod_recv, mod, proj, qsend, kvsend, qbuf, kvbuf, keys, q4,
    score_buf, near, whole, osend, mixed, marks, ranks,
    load_sem, mod_ssem, mod_rsem, q_ssem, q_rsem, kv_ssem, kv_rsem, qf_ssem, qf_rsem, kvf_ssem, kvf_rsem,
    wh_sem, o_ssem, o_rsem,
):
    me = lax.axis_index("tile")
    grp = lax.axis_index("grp")
    chip = me // 2
    core = me % 2
    sibling = me + 1 - 2 * core

    barrier = pltpu.get_barrier_semaphore()
    for off in ORDER:
        pl.semaphore_signal(
            barrier, inc=1, device_id={"tile": ((chip + off) % HEADS) * 2 + core}, device_id_type=MESH
        )
    for off in range(1, GROUPS):
        pl.semaphore_signal(barrier, inc=1, device_id={"grp": (grp + off) % GROUPS}, device_id_type=MESH)
    pl.semaphore_signal(barrier, inc=1, device_id={"tile": sibling}, device_id_type=MESH)

    load_c = pltpu.make_async_copy(cond_hbm, cond, load_sem.at[6])
    load_m = pltpu.make_async_copy(wm_hbm, wm, load_sem.at[0])
    load_x = pltpu.make_async_copy(x_hbm, x_ref, load_sem.at[1])
    load_d = pltpu.make_async_copy(marks_hbm, marks, load_sem.at[7])
    load_p = [
        pltpu.make_async_copy(wp_hbm.at[:, pl.ds(D * i, D)], wp.at[i], load_sem.at[2 + i]) for i in range(3)
    ]
    load_o = pltpu.make_async_copy(wo_hbm, wo, load_sem.at[5])
    for copy in (load_c, load_m, load_x, load_d):
        copy.start()

    mod_cols[...] = jnp.zeros_like(mod_cols)
    mod_send[...] = jnp.zeros_like(mod_send)
    mod[...] = jnp.zeros_like(mod)
    load_c.wait()
    load_m.wait()
    for copy in load_p + [load_o]:
        copy.start()
    mod_cols[:, :COLS] = lax.dot_general(
        cond[...], wm[...], (((1,), (1,)), ((), ())), preferred_element_type=F32
    )
    shifted = pltpu.roll(mod_cols[...], (grp * COLS) % 128, axis=1)
    for i in range(TILE_ROWS):
        mod_send[:, i, :] = shifted[:, i * 128 : (i + 1) * 128]

    pl.semaphore_wait(barrier, GROUPS - 1 + HEADS - 1 + 1)

    mod_copies = []
    for off in range(1, GROUPS):
        image = (grp + off) % GROUPS
        copy = pltpu.make_async_remote_copy(
            src_ref=mod_send.at[image], dst_ref=mod_recv.at[off - 1],
            send_sem=mod_ssem.at[off - 1], recv_sem=mod_rsem.at[off - 1],
            device_id={"grp": image}, device_id_type=MESH,
        )
        copy.start()
        mod_copies.append(copy)

    load_x.wait()
    values32 = x_ref[...].astype(F32)
    mean = jnp.mean(values32, axis=1, keepdims=True)
    centered = values32 - mean
    variance = jnp.mean(centered * centered, axis=1, keepdims=True)
    unit = centered / jnp.sqrt(variance + 1e-06)

    load_d.wait()
    rank = jnp.int32(0)
    slots = [jnp.int32(0)] * SIDE
    for t in range(TILES):
        mark = marks[0, t]
        for j in range(SIDE):
            hit = jnp.logical_and(mark > 0, rank == core * SIDE + j)
            slots[j] = jnp.where(hit, jnp.int32(t), slots[j])
        ranks[t] = jnp.minimum(rank, SLOTS - 1)
        rank = rank + mark

    def add_columns(source, block):
        rows = pl.ds((source * COLS) // 128, TILE_ROWS)
        mod[rows, :] += block[0:TILE_ROWS]

    add_columns(grp, mod_send[grp])
    for off in range(1, GROUPS):
        mod_copies[off - 1].wait_recv()
        add_columns((grp + GROUPS - off) % GROUPS, mod_recv[off - 1])

    def mod_row(part):
        first = part * D // 128
        return jnp.concatenate([mod[first + i : first + i + 1, :] for i in range(D // 128)], axis=1)

    normed = (unit * (1.0 + mod_row(1)) + mod_row(0)).astype(BF16)

    def project(part):
        load_p[part].wait()
        proj[part] = jnp.dot(normed, wp[part], preferred_element_type=F32).T

    def exchange(off, src, dst, ssem, rsem):
        other = (chip + off) % HEADS
        copy = pltpu.make_async_remote_copy(
            src_ref=src.at[other], dst_ref=dst, send_sem=ssem.at[off], recv_sem=rsem.at[off],
            device_id={"tile": other * 2 + core}, device_id_type=MESH,
        )
        copy.start()
        return copy

    def forward(off, src, dst, ssem, rsem):
        copy = pltpu.make_async_remote_copy(
            src_ref=src, dst_ref=dst.at[strip_of(off, core)], send_sem=ssem.at[off], recv_sem=rsem.at[off],
            device_id={"tile": sibling}, device_id_type=MESH,
        )
        copy.start()
        return copy

    def strip_of(off, parity):
        return ((chip + HEADS - off) % HEADS) * 2 + parity

    project(0)
    for h in range(HEADS):
        qsend[h] = jnp.concatenate(
            [proj[0, h * HEAD : (h + 1) * HEAD, :], jnp.zeros((PAD - HEAD, STRIP), F32)], axis=0
        ).astype(BF16)
    q_sent = [exchange(off, qsend, qbuf.at[me], q_ssem, q_rsem) for off in ORDER]
    q_passed = [forward(0, qsend.at[chip], qbuf, qf_ssem, qf_rsem)]
    qbuf[me] = qsend[chip]
    project(1)
    project(2)
    for h in range(HEADS):
        rows = slice(h * HEAD, (h + 1) * HEAD)
        kvsend[h] = jnp.concatenate([proj[1, rows, :], proj[2, rows, :]], axis=0).astype(BF16)
    kv_sent = []
    kv_passed = [forward(0, kvsend.at[chip], kvbuf, kvf_ssem, kvf_rsem)]
    kvbuf[me] = kvsend[chip]
    keys[pl.ds(0, STRIP), :] = jnp.zeros((STRIP, PAD), BF16)
    keys[pl.ds((TILES + 1) * STRIP, STRIP), :] = jnp.zeros((STRIP, PAD), BF16)

    for off, copy in zip(ORDER, q_sent):
        copy.wait_send()
        kv_sent.append(exchange(off, kvsend, kvbuf.at[me], kv_ssem, kv_rsem))
    for off, copy in zip(ORDER, q_sent):
        copy.wait_recv()
        q_passed.append(forward(off, qbuf.at[strip_of(off, core)], qbuf, qf_ssem, qf_rsem))
    for copy in q_passed:
        copy.wait_recv()
    for j in range(SIDE):
        q4[:, j * STRIP : (j + 1) * STRIP] = qbuf[slots[j]]

    def pair_of(off):
        return (chip + HEADS - off) % HEADS

    def scores_step(i, off, top):
        pair = pair_of(off)
        for parity in range(2):
            strip = pair * 2 + parity
            block = kvbuf[strip, 0:PAD, :].astype(F32).T
            keys[pl.ds(pl.multiple_of((strip + 1) * STRIP, STRIP), STRIP), :] = block.astype(BF16)
        block = keys[pl.ds(pl.multiple_of((2 * pair + 1) * STRIP, STRIP), 2 * STRIP), :]
        scores = jnp.dot(block, q4[...], preferred_element_type=F32)
        score_buf[i % 2] = scores
        return jnp.maximum(top, jnp.max(scores, axis=0, keepdims=True))

    def values_step(i, off, before, top, total, acc):
        pair = pair_of(off)
        factor = jnp.exp2((before - top) * EXP_SCALE)
        probs = jnp.exp2((score_buf[i % 2] - top) * EXP_SCALE)
        total = total * factor + jnp.sum(probs, axis=0, keepdims=True)
        rows = slice(V_AT, V_AT + PAD)
        values = jnp.concatenate([kvbuf[2 * pair, rows, :], kvbuf[2 * pair + 1, rows, :]], axis=1)
        acc = acc * factor + jnp.dot(values, probs.astype(BF16), preferred_element_type=F32)
        return total, acc

    def near_step(off):
        pair = pair_of(off)
        strip = 2 * pair + core
        block = keys[pl.ds(pl.multiple_of((strip + 1) * STRIP - MARGIN, MARGIN), 2 * STRIP), :]
        scores = jnp.dot(block, qbuf[strip], preferred_element_type=F32)
        at = strip * STRIP - MARGIN + lax.broadcasted_iota(jnp.int32, scores.shape, 0)
        scores = jnp.where(jnp.logical_and(at >= 0, at < TILES * STRIP), scores, -1e30)
        probs = jnp.exp2((scores - jnp.max(scores, axis=0, keepdims=True)) * EXP_SCALE)
        sums = jnp.sum(probs, axis=0, keepdims=True)
        blank = jnp.zeros((MARGIN, STRIP), BF16)
        weights = jnp.concatenate([blank, probs.astype(BF16), blank], axis=0)
        rows = pl.ds(V_AT, PAD)
        values = jnp.concatenate(
            [
                kvbuf[jnp.maximum(strip - 1, 0), rows, :],
                kvbuf[strip, rows, :],
                kvbuf[jnp.minimum(strip + 1, TILES - 1), rows, :],
            ],
            axis=1,
        )
        near[pair] = (jnp.dot(values, weights, preferred_element_type=F32) / sums)[8:PAD]

    steps = (0,) + ORDER
    total = jnp.zeros((1, WIDE), F32)
    acc = jnp.zeros((PAD, WIDE), F32)
    tops = [jnp.full((1, WIDE), -1e30, F32)]
    ready = []
    done = 0
    for i, off in enumerate(steps):
        while len(kv_passed) < min(i + AHEAD + 1, len(steps)):
            kv_sent[len(kv_passed) - 1].wait_recv()
            later = steps[len(kv_passed)]
            kv_passed.append(forward(later, kvbuf.at[strip_of(later, core)], kvbuf, kvf_ssem, kvf_rsem))
        kv_passed[i].wait_recv()
        tops.append(scores_step(i, off, tops[i]))
        if i > 0:
            total, acc = values_step(i - 1, steps[i - 1], tops[i - 1], tops[i], total, acc)
            if i + 1 < len(steps):
                for strip_off in ready[done:]:
                    near_step(strip_off)
                done = len(ready)
        come = steps[: i + 1]
        for o in come:
            if o not in ready and (o + 1) % HEADS in come and (o - 1) % HEADS in come:
                ready.append(o)
    last = len(steps) - 1
    total, acc = values_step(last, steps[last], tops[last], tops[last + 1], total, acc)
    result = acc / total
    for j in range(SIDE):
        whole[core * SIDE + j] = result[8:PAD, j * STRIP : (j + 1) * STRIP]
    mine = whole.at[pl.ds(core * SIDE, SIDE)]
    swap = pltpu.make_async_remote_copy(
        src_ref=mine, dst_ref=mine, send_sem=wh_sem.at[0], recv_sem=wh_sem.at[1],
        device_id={"tile": sibling}, device_id_type=MESH,
    )
    swap.start()
    for strip_off in ready[done:]:
        near_step(strip_off)
    swap.wait_recv()

    for j in range(TILES // 2):
        strip = 2 * j + core
        extra = whole[ranks[strip]]
        total = near[j] + jnp.where(marks[0, strip] > 0, extra, 0.0)
        osend[j] = jnp.concatenate(
            [total[8 * r : 8 * r + 8] for r in range(HEAD // 8)], axis=1
        ).astype(BF16)
    outs = [exchange(off, osend, mixed.at[chip], o_ssem, o_rsem) for off in ORDER]
    mixed[chip] = osend[chip]
    load_o.wait()
    for copy in outs:
        copy.wait_recv()

    gathered = []
    for h in range(HEADS):
        block = mixed[h].astype(F32)
        gathered += [block[:, 128 * r : 128 * r + 128] for r in range(HEAD // 8)]
    gathered = jnp.concatenate(gathered, axis=0).T
    branch = jnp.dot(gathered.astype(BF16), wo[...], preferred_element_type=F32)
    out_ref[...] = (x_ref[...].astype(F32) + mod_row(2) * branch).astype(BF16)

    for copy in mod_copies + q_passed + kv_sent + kv_passed + outs + [swap]:
        copy.wait_send()


def on_device(latents, condition, w_modulate, w_project, w_output, detail):
    hbm = pl.BlockSpec(memory_space=pl.ANY)
    dma = pltpu.SemaphoreType.DMA
    updated = pl.pallas_call(
        body,
        out_shape=pltpu.VMEM((STRIP, D), BF16),
        in_specs=[hbm] * 6,
        out_specs=pl.BlockSpec(memory_space=pltpu.VMEM),
        scratch_shapes=[
            pltpu.VMEM((STRIP, D), BF16),
            pltpu.VMEM((GROUPS, D), BF16),
            pltpu.VMEM((COLS, D), BF16),
            pltpu.VMEM((3, D, D), BF16),
            pltpu.VMEM((D, D), BF16),
            pltpu.VMEM((GROUPS, SPAN), F32),
            pltpu.VMEM((GROUPS, 8, 128), F32),
            pltpu.VMEM((GROUPS - 1, 8, 128), F32),
            pltpu.VMEM((32, 128), F32),
            pltpu.VMEM((3, D, STRIP), F32),
            pltpu.VMEM((HEADS, PAD, STRIP), BF16),
            pltpu.VMEM((HEADS, 2 * HEAD, STRIP), BF16),
            pltpu.VMEM((TILES, PAD, STRIP), BF16),
            pltpu.VMEM((TILES, 2 * HEAD, STRIP), BF16),
            pltpu.VMEM(((TILES + 2) * STRIP, PAD), BF16),
            pltpu.VMEM((PAD, WIDE), BF16),
            pltpu.VMEM((2, 2 * STRIP, WIDE), F32),
            pltpu.VMEM((TILES // 2, HEAD, STRIP), F32),
            pltpu.VMEM((SLOTS, HEAD, STRIP), F32),
            pltpu.VMEM((HEADS, 8, D), BF16),
            pltpu.VMEM((HEADS, 8, D), BF16),
            pltpu.SMEM((1, TILES), jnp.int32),
            pltpu.SMEM((TILES,), jnp.int32),
            dma((8,)),
            dma((GROUPS - 1,)), dma((GROUPS - 1,)),
            dma((HEADS,)), dma((HEADS,)),
            dma((HEADS,)), dma((HEADS,)),
            dma((HEADS,)), dma((HEADS,)),
            dma((HEADS,)), dma((HEADS,)),
            dma((2,)),
            dma((HEADS,)), dma((HEADS,)),
        ],
        compiler_params=pltpu.CompilerParams(
            collective_id=0, has_side_effects=True, vmem_limit_bytes=56 * 1024 * 1024
        ),
    )(latents[0], condition, w_modulate.T, w_project, w_output, detail)
    return updated[None]


def solution(mesh):
    in_specs = (P("grp", "tile", None), P(), P(None, "grp"), P(), P(), P("grp", None))
    out_specs = P("grp", "tile", None)
    return jax.shard_map(
        on_device, mesh=mesh, in_specs=in_specs, out_specs=out_specs, check_vma=False
    )
```

```python
import functools

import jax
import jax.numpy as jnp
from jax import lax
from jax.experimental import pallas as pl
from jax.experimental.pallas import tpu as pltpu
from jax.sharding import PartitionSpec as P

HEADS = 16
HEAD = 72
D = HEADS * HEAD
STRIP = 128
MARGIN = 64
TILES = 32
SLOTS = 8
GROUPS = 8
COLS = 3 * D // GROUPS
SPAN = 640
PAD = 80
V_AT = HEAD - 8
SIDE = SLOTS // 2
WIDE = SIDE * STRIP
TILE_ROWS = 5
AHEAD = 2
EXP_SCALE = 1.4426950408889634 / (HEAD ** 0.5)
MESH = pl.DeviceIdType.MESH
F32 = jnp.float32
BF16 = jnp.bfloat16
ORDER = (1, 15, 3, 14, 2, 5, 13, 4, 12, 11, 7, 10, 6, 9, 8)
PARTS = (0, 128, 256, COLS)


def side_by_side(block):
    return jnp.concatenate([block[8 * r : 8 * r + 8] for r in range(HEAD // 8)], axis=1).astype(BF16)


def stacked(message):
    block = message.astype(F32)
    return [block[:, 128 * r : 128 * r + 128] for r in range(HEAD // 8)]


def queries(message):
    return jnp.concatenate(stacked(message) + [jnp.zeros((PAD - HEAD, STRIP), F32)], axis=0).astype(BF16)


def body(
    x_hbm, cond_hbm, wm_hbm, wp_hbm, wo_hbm, marks_hbm,
    out_ref,
    x_ref, cond, wm, wp, wo, mod_cols, mod_send, mod_recv, mod, proj, qsend, kvsend, qbuf, kvbuf, keys, q4,
    score_buf, near, whole, branch, osend, mixed, marks, ranks,
    load_sem, mod_ssem, mod_rsem, q_ssem, q_rsem, kv_ssem, kv_rsem, qf_ssem, qf_rsem, kvf_ssem, kvf_rsem,
    wh_sem, o_ssem, o_rsem,
):
    me = lax.axis_index("tile")
    grp = lax.axis_index("grp")
    chip = me // 2
    core = me % 2
    sibling = me + 1 - 2 * core

    barrier = pltpu.get_barrier_semaphore()
    for off in ORDER:
        pl.semaphore_signal(
            barrier, inc=1, device_id={"tile": ((chip + off) % HEADS) * 2 + core}, device_id_type=MESH
        )
    for off in range(1, GROUPS):
        pl.semaphore_signal(barrier, inc=1, device_id={"grp": (grp + off) % GROUPS}, device_id_type=MESH)
    pl.semaphore_signal(barrier, inc=1, device_id={"tile": sibling}, device_id_type=MESH)

    load_c = pltpu.make_async_copy(cond_hbm, cond, load_sem.at[6])
    load_m = [
        pltpu.make_async_copy(wm_hbm.at[pl.ds(a, b - a)], wm.at[pl.ds(a, b - a)], load_sem.at[8 + i])
        for i, (a, b) in enumerate(zip(PARTS, PARTS[1:]))
    ]
    load_x = pltpu.make_async_copy(x_hbm, x_ref, load_sem.at[1])
    load_d = pltpu.make_async_copy(marks_hbm, marks, load_sem.at[7])
    load_p = [
        pltpu.make_async_copy(wp_hbm.at[:, pl.ds(D * i, D)], wp.at[i], load_sem.at[2 + i]) for i in range(3)
    ]
    load_o = pltpu.make_async_copy(wo_hbm, wo, load_sem.at[5])
    for copy in [load_c] + load_m + [load_x, load_d]:
        copy.start()

    mod_cols[...] = jnp.zeros_like(mod_cols)
    mod_send[...] = jnp.zeros_like(mod_send)
    mod[...] = jnp.zeros_like(mod)
    load_c.wait()
    for copy in load_m:
        copy.wait()
    for copy in load_p + [load_o]:
        copy.start()
    mod_cols[:, :COLS] = lax.dot_general(
        cond[...], wm[...], (((1,), (1,)), ((), ())), preferred_element_type=F32
    )
    shifted = pltpu.roll(mod_cols[...], (grp * COLS) % 128, axis=1)
    for i in range(TILE_ROWS):
        mod_send[:, i, :] = shifted[:, i * 128 : (i + 1) * 128]

    pl.semaphore_wait(barrier, GROUPS - 1 + HEADS - 1 + 1)

    mod_copies = []
    for off in range(1, GROUPS):
        image = (grp + off) % GROUPS
        copy = pltpu.make_async_remote_copy(
            src_ref=mod_send.at[image], dst_ref=mod_recv.at[off - 1],
            send_sem=mod_ssem.at[off - 1], recv_sem=mod_rsem.at[off - 1],
            device_id={"grp": image}, device_id_type=MESH,
        )
        copy.start()
        mod_copies.append(copy)

    load_x.wait()
    values32 = x_ref[...].astype(F32)
    mean = jnp.mean(values32, axis=1, keepdims=True)
    centered = values32 - mean
    variance = jnp.mean(centered * centered, axis=1, keepdims=True)
    unit = centered / jnp.sqrt(variance + 1e-06)

    load_d.wait()
    rank = jnp.int32(0)
    slots = [jnp.int32(0)] * SIDE
    for t in range(TILES):
        mark = marks[0, t]
        for j in range(SIDE):
            hit = jnp.logical_and(mark > 0, rank == core * SIDE + j)
            slots[j] = jnp.where(hit, jnp.int32(t), slots[j])
        ranks[t] = jnp.minimum(rank, SLOTS - 1)
        rank = rank + mark

    def add_columns(source, block):
        rows = pl.ds((source * COLS) // 128, TILE_ROWS)
        mod[rows, :] += block[0:TILE_ROWS]

    add_columns(grp, mod_send[grp])
    for off in range(1, GROUPS):
        mod_copies[off - 1].wait_recv()
        add_columns((grp + GROUPS - off) % GROUPS, mod_recv[off - 1])

    def mod_row(part):
        first = part * D // 128
        return jnp.concatenate([mod[first + i : first + i + 1, :] for i in range(D // 128)], axis=1)

    normed = (unit * (1.0 + mod_row(1)) + mod_row(0)).astype(BF16)

    def project(part):
        load_p[part].wait()
        proj[part] = jnp.dot(normed, wp[part], preferred_element_type=F32).T

    def exchange(off, src, dst, ssem, rsem):
        other = (chip + off) % HEADS
        copy = pltpu.make_async_remote_copy(
            src_ref=src.at[other], dst_ref=dst, send_sem=ssem.at[off], recv_sem=rsem.at[off],
            device_id={"tile": other * 2 + core}, device_id_type=MESH,
        )
        copy.start()
        return copy

    def forward(off, src, dst, ssem, rsem):
        copy = pltpu.make_async_remote_copy(
            src_ref=src, dst_ref=dst.at[strip_of(off, core)], send_sem=ssem.at[off], recv_sem=rsem.at[off],
            device_id={"tile": sibling}, device_id_type=MESH,
        )
        copy.start()
        return copy

    def strip_of(off, parity):
        return ((chip + HEADS - off) % HEADS) * 2 + parity

    project(0)
    for h in range(HEADS):
        qsend[h] = side_by_side(proj[0, h * HEAD : (h + 1) * HEAD, :])
    q_sent = [exchange(off, qsend, qbuf.at[me], q_ssem, q_rsem) for off in ORDER]
    q_passed = [forward(0, qsend.at[chip], qbuf, qf_ssem, qf_rsem)]
    qbuf[me] = qsend[chip]
    project(1)
    project(2)
    for h in range(HEADS):
        rows = slice(h * HEAD, (h + 1) * HEAD)
        kvsend[h] = jnp.concatenate([proj[1, rows, :], proj[2, rows, :]], axis=0).astype(BF16)
    kv_sent = []
    kv_passed = [forward(0, kvsend.at[chip], kvbuf, kvf_ssem, kvf_rsem)]
    kvbuf[me] = kvsend[chip]
    keys[pl.ds(0, STRIP), :] = jnp.zeros((STRIP, PAD), BF16)
    keys[pl.ds((TILES + 1) * STRIP, STRIP), :] = jnp.zeros((STRIP, PAD), BF16)

    for off, copy in zip(ORDER, q_sent):
        copy.wait_send()
        kv_sent.append(exchange(off, kvsend, kvbuf.at[me], kv_ssem, kv_rsem))
    for off, copy in zip(ORDER, q_sent):
        copy.wait_recv()
        q_passed.append(forward(off, qbuf.at[strip_of(off, core)], qbuf, qf_ssem, qf_rsem))
    for copy in q_passed:
        copy.wait_recv()
    for j in range(SIDE):
        q4[:, j * STRIP : (j + 1) * STRIP] = queries(qbuf[slots[j]])

    def pair_of(off):
        return (chip + HEADS - off) % HEADS

    def scores_step(i, off, top):
        pair = pair_of(off)
        for parity in range(2):
            strip = pair * 2 + parity
            block = kvbuf[strip, 0:PAD, :].astype(F32).T
            keys[pl.ds(pl.multiple_of((strip + 1) * STRIP, STRIP), STRIP), :] = block.astype(BF16)
        block = keys[pl.ds(pl.multiple_of((2 * pair + 1) * STRIP, STRIP), 2 * STRIP), :]
        scores = jnp.dot(block, q4[...], preferred_element_type=F32)
        score_buf[i % 2] = scores
        return jnp.maximum(top, jnp.max(scores, axis=0, keepdims=True))

    def values_step(i, off, before, top, total, acc):
        pair = pair_of(off)
        factor = jnp.exp2((before - top) * EXP_SCALE)
        probs = jnp.exp2((score_buf[i % 2] - top) * EXP_SCALE)
        total = total * factor + jnp.sum(probs, axis=0, keepdims=True)
        rows = slice(V_AT, V_AT + PAD)
        values = jnp.concatenate([kvbuf[2 * pair, rows, :], kvbuf[2 * pair + 1, rows, :]], axis=1)
        acc = acc * factor + jnp.dot(values, probs.astype(BF16), preferred_element_type=F32)
        return total, acc

    def near_step(off):
        pair = pair_of(off)
        strip = 2 * pair + core
        block = keys[pl.ds(pl.multiple_of((strip + 1) * STRIP - MARGIN, MARGIN), 2 * STRIP), :]
        scores = jnp.dot(block, queries(qbuf[strip]), preferred_element_type=F32)
        at = strip * STRIP - MARGIN + lax.broadcasted_iota(jnp.int32, scores.shape, 0)
        scores = jnp.where(jnp.logical_and(at >= 0, at < TILES * STRIP), scores, -1e30)
        probs = jnp.exp2((scores - jnp.max(scores, axis=0, keepdims=True)) * EXP_SCALE)
        sums = jnp.sum(probs, axis=0, keepdims=True)
        blank = jnp.zeros((MARGIN, STRIP), BF16)
        weights = jnp.concatenate([blank, probs.astype(BF16), blank], axis=0)
        rows = pl.ds(V_AT, PAD)
        values = jnp.concatenate(
            [
                kvbuf[jnp.maximum(strip - 1, 0), rows, :],
                kvbuf[strip, rows, :],
                kvbuf[jnp.minimum(strip + 1, TILES - 1), rows, :],
            ],
            axis=1,
        )
        near[pair] = (jnp.dot(values, weights, preferred_element_type=F32) / sums)[8:PAD]

    steps = (0,) + ORDER
    total = jnp.zeros((1, WIDE), F32)
    acc = jnp.zeros((PAD, WIDE), F32)
    tops = [jnp.full((1, WIDE), -1e30, F32)]
    ready = []
    done = 0
    for i, off in enumerate(steps):
        while len(kv_passed) < min(i + AHEAD + 1, len(steps)):
            kv_sent[len(kv_passed) - 1].wait_recv()
            later = steps[len(kv_passed)]
            kv_passed.append(forward(later, kvbuf.at[strip_of(later, core)], kvbuf, kvf_ssem, kvf_rsem))
        kv_passed[i].wait_recv()
        tops.append(scores_step(i, off, tops[i]))
        if i > 0:
            total, acc = values_step(i - 1, steps[i - 1], tops[i - 1], tops[i], total, acc)
            if i + 1 < len(steps):
                for strip_off in ready[done:]:
                    near_step(strip_off)
                done = len(ready)
        come = steps[: i + 1]
        for o in come:
            if o not in ready and (o + 1) % HEADS in come and (o - 1) % HEADS in come:
                ready.append(o)
    last = len(steps) - 1
    total, acc = values_step(last, steps[last], tops[last], tops[last + 1], total, acc)
    result = acc / total
    for j in range(SIDE):
        whole[core * SIDE + j] = result[8:PAD, j * STRIP : (j + 1) * STRIP]
    mine = whole.at[pl.ds(core * SIDE, SIDE)]
    swap = pltpu.make_async_remote_copy(
        src_ref=mine, dst_ref=mine, send_sem=wh_sem.at[0], recv_sem=wh_sem.at[1],
        device_id={"tile": sibling}, device_id_type=MESH,
    )
    swap.start()
    for strip_off in ready[done:]:
        near_step(strip_off)
    swap.wait_recv()

    for j in range(TILES // 2):
        strip = 2 * j + core
        extra = whole[ranks[strip]]
        total = near[j] + jnp.where(marks[0, strip] > 0, extra, 0.0)
        osend[j] = side_by_side(total)
    outs = [exchange(off, osend, mixed.at[chip], o_ssem, o_rsem) for off in ORDER]
    mixed[chip] = osend[chip]
    load_o.wait()

    def project_head(head):
        block = jnp.concatenate(stacked(mixed[head]), axis=0).T
        return jnp.dot(block.astype(BF16), wo[head], preferred_element_type=F32)

    branch[...] = project_head(chip)
    for off, copy in zip(ORDER, outs):
        copy.wait_recv()
        if off != ORDER[-1]:
            branch[...] += project_head((chip + HEADS - off) % HEADS)
    result = branch[...] + project_head((chip + HEADS - ORDER[-1]) % HEADS)
    out_ref[...] = (x_ref[...].astype(F32) + mod_row(2) * result).astype(BF16)

    for copy in mod_copies + q_passed + kv_sent + kv_passed + outs + [swap]:
        copy.wait_send()


def on_device(latents, condition, w_modulate, w_project, w_output, detail):
    hbm = pl.BlockSpec(memory_space=pl.ANY)
    dma = pltpu.SemaphoreType.DMA
    updated = pl.pallas_call(
        body,
        out_shape=pltpu.VMEM((STRIP, D), BF16),
        in_specs=[hbm] * 6,
        out_specs=pl.BlockSpec(memory_space=pltpu.VMEM),
        scratch_shapes=[
            pltpu.VMEM((STRIP, D), BF16),
            pltpu.VMEM((GROUPS, D), BF16),
            pltpu.VMEM((COLS, D), BF16),
            pltpu.VMEM((3, D, D), BF16),
            pltpu.VMEM((HEADS, HEAD, D), BF16),
            pltpu.VMEM((GROUPS, SPAN), F32),
            pltpu.VMEM((GROUPS, 8, 128), F32),
            pltpu.VMEM((GROUPS - 1, 8, 128), F32),
            pltpu.VMEM((32, 128), F32),
            pltpu.VMEM((3, D, STRIP), F32),
            pltpu.VMEM((HEADS, 8, D), BF16),
            pltpu.VMEM((HEADS, 2 * HEAD, STRIP), BF16),
            pltpu.VMEM((TILES, 8, D), BF16),
            pltpu.VMEM((TILES, 2 * HEAD, STRIP), BF16),
            pltpu.VMEM(((TILES + 2) * STRIP, PAD), BF16),
            pltpu.VMEM((PAD, WIDE), BF16),
            pltpu.VMEM((2, 2 * STRIP, WIDE), F32),
            pltpu.VMEM((TILES // 2, HEAD, STRIP), F32),
            pltpu.VMEM((SLOTS, HEAD, STRIP), F32),
            pltpu.VMEM((STRIP, D), F32),
            pltpu.VMEM((HEADS, 8, D), BF16),
            pltpu.VMEM((HEADS, 8, D), BF16),
            pltpu.SMEM((1, TILES), jnp.int32),
            pltpu.SMEM((TILES,), jnp.int32),
            dma((11,)),
            dma((GROUPS - 1,)), dma((GROUPS - 1,)),
            dma((HEADS,)), dma((HEADS,)),
            dma((HEADS,)), dma((HEADS,)),
            dma((HEADS,)), dma((HEADS,)),
            dma((HEADS,)), dma((HEADS,)),
            dma((2,)),
            dma((HEADS,)), dma((HEADS,)),
        ],
        compiler_params=pltpu.CompilerParams(
            collective_id=0, has_side_effects=True, vmem_limit_bytes=56 * 1024 * 1024
        ),
    )(latents[0], condition, w_modulate.T, w_project, w_output.reshape(HEADS, HEAD, D), detail)
    return updated[None]


def solution(mesh):
    in_specs = (P("grp", "tile", None), P(), P(None, "grp"), P(), P(), P("grp", None))
    out_specs = P("grp", "tile", None)
    return jax.shard_map(
        on_device, mesh=mesh, in_specs=in_specs, out_specs=out_specs, check_vma=False
    )
```

```python
import functools

import jax
import jax.numpy as jnp
from jax import lax
from jax.experimental import pallas as pl
from jax.experimental.pallas import tpu as pltpu
from jax.sharding import PartitionSpec as P

HEADS = 16
HEAD = 72
D = HEADS * HEAD
STRIP = 128
MARGIN = 64
TILES = 32
SLOTS = 8
GROUPS = 8
COLS = 3 * D // GROUPS
SPAN = 640
PAD = 80
V_AT = HEAD - 8
SIDE = SLOTS // 2
WIDE = SIDE * STRIP
TILE_ROWS = 5
AHEAD = 2
EARLY = 9
EXP_SCALE = 1.4426950408889634 / (HEAD ** 0.5)
MESH = pl.DeviceIdType.MESH
F32 = jnp.float32
BF16 = jnp.bfloat16
ORDER = (1, 15, 3, 14, 2, 5, 13, 4, 12, 11, 7, 10, 6, 9, 8)
PARTS = (0, 128, 256, COLS)


def side_by_side(block):
    return jnp.concatenate([block[8 * r : 8 * r + 8] for r in range(HEAD // 8)], axis=1).astype(BF16)


def stacked(message):
    block = message.astype(F32)
    return [block[:, 128 * r : 128 * r + 128] for r in range(HEAD // 8)]


def queries(message):
    return jnp.concatenate(stacked(message) + [jnp.zeros((PAD - HEAD, STRIP), F32)], axis=0).astype(BF16)


def body(
    x_hbm, cond_hbm, wm_hbm, wp_hbm, wo_hbm, marks_hbm,
    out_ref,
    x_ref, cond, wm, wp, wo, mod_cols, mod_send, mod_recv, mod, proj, qsend, kvsend, qbuf, kvbuf, keys, q4,
    score_buf, near, whole, branch, osend, mixed, marks, ranks,
    load_sem, mod_ssem, mod_rsem, q_ssem, q_rsem, kv_ssem, kv_rsem, qf_ssem, qf_rsem, kvf_ssem, kvf_rsem,
    wh_sem, o_ssem, o_rsem, rounds,
):
    me = lax.axis_index("tile")
    grp = lax.axis_index("grp")
    chip = me // 2
    core = me % 2
    sibling = me + 1 - 2 * core

    barrier = pltpu.get_barrier_semaphore()
    around = [(me + 4) % TILES, (me + TILES - 4) % TILES]
    for near_by in around + [me + 2 - 4 * (chip % 2), sibling]:
        pl.semaphore_signal(barrier, inc=1, device_id={"tile": near_by}, device_id_type=MESH)
    for off in range(1, GROUPS):
        pl.semaphore_signal(barrier, inc=1, device_id={"grp": (grp + off) % GROUPS}, device_id_type=MESH)

    def tell(step):
        for near_by in around:
            pl.semaphore_signal(rounds.at[step], inc=1, device_id={"tile": near_by}, device_id_type=MESH)

    def hear(step):
        pl.semaphore_wait(rounds.at[step], 2)

    load_c = pltpu.make_async_copy(cond_hbm, cond, load_sem.at[6])
    load_m = [
        pltpu.make_async_copy(wm_hbm.at[pl.ds(a, b - a)], wm.at[pl.ds(a, b - a)], load_sem.at[8 + i])
        for i, (a, b) in enumerate(zip(PARTS, PARTS[1:]))
    ]
    load_x = pltpu.make_async_copy(x_hbm, x_ref, load_sem.at[1])
    load_d = pltpu.make_async_copy(marks_hbm, marks, load_sem.at[7])
    load_p = [
        pltpu.make_async_copy(wp_hbm.at[:, pl.ds(D * i, D)], wp.at[i], load_sem.at[2 + i]) for i in range(3)
    ]
    load_o = pltpu.make_async_copy(wo_hbm, wo, load_sem.at[5])
    for copy in [load_c] + load_m + [load_x, load_d]:
        copy.start()

    mod_cols[...] = jnp.zeros_like(mod_cols)
    mod_send[...] = jnp.zeros_like(mod_send)
    mod[...] = jnp.zeros_like(mod)
    load_c.wait()
    for copy in load_m:
        copy.wait()
    for copy in load_p + [load_o]:
        copy.start()
    mod_cols[:, :COLS] = lax.dot_general(
        cond[...], wm[...], (((1,), (1,)), ((), ())), preferred_element_type=F32
    )
    shifted = pltpu.roll(mod_cols[...], (grp * COLS) % 128, axis=1)
    for i in range(TILE_ROWS):
        mod_send[:, i, :] = shifted[:, i * 128 : (i + 1) * 128]

    pl.semaphore_wait(barrier, GROUPS - 1 + 4)

    mod_copies = []
    for off in range(1, GROUPS):
        image = (grp + off) % GROUPS
        copy = pltpu.make_async_remote_copy(
            src_ref=mod_send.at[image], dst_ref=mod_recv.at[off - 1],
            send_sem=mod_ssem.at[off - 1], recv_sem=mod_rsem.at[off - 1],
            device_id={"grp": image}, device_id_type=MESH,
        )
        copy.start()
        mod_copies.append(copy)

    tell(0)
    load_x.wait()
    values32 = x_ref[...].astype(F32)
    mean = jnp.mean(values32, axis=1, keepdims=True)
    centered = values32 - mean
    variance = jnp.mean(centered * centered, axis=1, keepdims=True)
    unit = centered / jnp.sqrt(variance + 1e-06)

    hear(0)
    tell(1)

    load_d.wait()
    rank = jnp.int32(0)
    slots = [jnp.int32(0)] * SIDE
    for t in range(TILES):
        mark = marks[0, t]
        for j in range(SIDE):
            hit = jnp.logical_and(mark > 0, rank == core * SIDE + j)
            slots[j] = jnp.where(hit, jnp.int32(t), slots[j])
        ranks[t] = jnp.minimum(rank, SLOTS - 1)
        rank = rank + mark

    hear(1)
    tell(2)

    def add_columns(source, block):
        rows = pl.ds((source * COLS) // 128, TILE_ROWS)
        mod[rows, :] += block[0:TILE_ROWS]

    add_columns(grp, mod_send[grp])
    hear(2)
    tell(3)
    for off in range(1, GROUPS):
        mod_copies[off - 1].wait_recv()
        add_columns((grp + GROUPS - off) % GROUPS, mod_recv[off - 1])

    def mod_row(part):
        first = part * D // 128
        return jnp.concatenate([mod[first + i : first + i + 1, :] for i in range(D // 128)], axis=1)

    normed = (unit * (1.0 + mod_row(1)) + mod_row(0)).astype(BF16)

    def project(part):
        load_p[part].wait()
        proj[part] = jnp.dot(normed, wp[part], preferred_element_type=F32).T

    def exchange(off, src, dst, ssem, rsem):
        other = (chip + off) % HEADS
        copy = pltpu.make_async_remote_copy(
            src_ref=src.at[other], dst_ref=dst, send_sem=ssem.at[off], recv_sem=rsem.at[off],
            device_id={"tile": other * 2 + core}, device_id_type=MESH,
        )
        copy.start()
        return copy

    def forward(off, src, dst, ssem, rsem):
        copy = pltpu.make_async_remote_copy(
            src_ref=src, dst_ref=dst.at[strip_of(off, core)], send_sem=ssem.at[off], recv_sem=rsem.at[off],
            device_id={"tile": sibling}, device_id_type=MESH,
        )
        copy.start()
        return copy

    def strip_of(off, parity):
        return ((chip + HEADS - off) % HEADS) * 2 + parity

    project(0)
    for h in range(HEADS):
        qsend[h] = side_by_side(proj[0, h * HEAD : (h + 1) * HEAD, :])
    hear(3)
    q_sent = [exchange(off, qsend, qbuf.at[me], q_ssem, q_rsem) for off in ORDER]
    q_passed = [forward(0, qsend.at[chip], qbuf, qf_ssem, qf_rsem)]
    qbuf[me] = qsend[chip]
    project(1)
    project(2)
    for h in range(HEADS):
        rows = slice(h * HEAD, (h + 1) * HEAD)
        kvsend[h] = jnp.concatenate([proj[1, rows, :], proj[2, rows, :]], axis=0).astype(BF16)
    kv_sent = []
    kv_passed = [forward(0, kvsend.at[chip], kvbuf, kvf_ssem, kvf_rsem)]
    kvbuf[me] = kvsend[chip]
    keys[pl.ds(0, STRIP), :] = jnp.zeros((STRIP, PAD), BF16)
    keys[pl.ds((TILES + 1) * STRIP, STRIP), :] = jnp.zeros((STRIP, PAD), BF16)

    for off, copy in zip(ORDER, q_sent):
        copy.wait_send()
        kv_sent.append(exchange(off, kvsend, kvbuf.at[me], kv_ssem, kv_rsem))
    for off, copy in zip(ORDER, q_sent):
        copy.wait_recv()
        q_passed.append(forward(off, qbuf.at[strip_of(off, core)], qbuf, qf_ssem, qf_rsem))
    for copy in q_passed:
        copy.wait_recv()
    for j in range(SIDE):
        q4[:, j * STRIP : (j + 1) * STRIP] = queries(qbuf[slots[j]])

    def pair_of(off):
        return (chip + HEADS - off) % HEADS

    def scores_step(i, off, top):
        pair = pair_of(off)
        for parity in range(2):
            strip = pair * 2 + parity
            block = kvbuf[strip, 0:PAD, :].astype(F32).T
            keys[pl.ds(pl.multiple_of((strip + 1) * STRIP, STRIP), STRIP), :] = block.astype(BF16)
        block = keys[pl.ds(pl.multiple_of((2 * pair + 1) * STRIP, STRIP), 2 * STRIP), :]
        scores = jnp.dot(block, q4[...], preferred_element_type=F32)
        score_buf[i % 2] = scores
        return jnp.maximum(top, jnp.max(scores, axis=0, keepdims=True))

    def values_step(i, off, before, top, total, acc):
        pair = pair_of(off)
        factor = jnp.exp2((before - top) * EXP_SCALE)
        probs = jnp.exp2((score_buf[i % 2] - top) * EXP_SCALE)
        total = total * factor + jnp.sum(probs, axis=0, keepdims=True)
        rows = slice(V_AT, V_AT + PAD)
        values = jnp.concatenate([kvbuf[2 * pair, rows, :], kvbuf[2 * pair + 1, rows, :]], axis=1)
        acc = acc * factor + jnp.dot(values, probs.astype(BF16), preferred_element_type=F32)
        return total, acc

    def near_step(off):
        pair = pair_of(off)
        strip = 2 * pair + core
        block = keys[pl.ds(pl.multiple_of((strip + 1) * STRIP - MARGIN, MARGIN), 2 * STRIP), :]
        scores = jnp.dot(block, queries(qbuf[strip]), preferred_element_type=F32)
        at = strip * STRIP - MARGIN + lax.broadcasted_iota(jnp.int32, scores.shape, 0)
        scores = jnp.where(jnp.logical_and(at >= 0, at < TILES * STRIP), scores, -1e30)
        probs = jnp.exp2((scores - jnp.max(scores, axis=0, keepdims=True)) * EXP_SCALE)
        sums = jnp.sum(probs, axis=0, keepdims=True)
        blank = jnp.zeros((MARGIN, STRIP), BF16)
        weights = jnp.concatenate([blank, probs.astype(BF16), blank], axis=0)
        rows = pl.ds(V_AT, PAD)
        values = jnp.concatenate(
            [
                kvbuf[jnp.maximum(strip - 1, 0), rows, :],
                kvbuf[strip, rows, :],
                kvbuf[jnp.minimum(strip + 1, TILES - 1), rows, :],
            ],
            axis=1,
        )
        near[pair] = (jnp.dot(values, weights, preferred_element_type=F32) / sums)[8:PAD]

    steps = (0,) + ORDER
    total = jnp.zeros((1, WIDE), F32)
    acc = jnp.zeros((PAD, WIDE), F32)
    tops = [jnp.full((1, WIDE), -1e30, F32)]
    ready = []
    done = 0
    for i, off in enumerate(steps):
        while len(kv_passed) < min(i + AHEAD + 1, len(steps)):
            kv_sent[len(kv_passed) - 1].wait_recv()
            later = steps[len(kv_passed)]
            kv_passed.append(forward(later, kvbuf.at[strip_of(later, core)], kvbuf, kvf_ssem, kvf_rsem))
        kv_passed[i].wait_recv()
        tops.append(scores_step(i, off, tops[i]))
        if i > 0:
            total, acc = values_step(i - 1, steps[i - 1], tops[i - 1], tops[i], total, acc)
            if i + 1 < len(steps):
                for strip_off in ready[done:]:
                    near_step(strip_off)
                done = len(ready)
        come = steps[: i + 1]
        for o in come:
            if o not in ready and (o + 1) % HEADS in come and (o - 1) % HEADS in come:
                ready.append(o)
    last = len(steps) - 1
    total, acc = values_step(last, steps[last], tops[last], tops[last + 1], total, acc)
    result = acc / total
    for j in range(SIDE):
        whole[core * SIDE + j] = result[8:PAD, j * STRIP : (j + 1) * STRIP]
    mine = whole.at[pl.ds(core * SIDE, SIDE)]
    swap = pltpu.make_async_remote_copy(
        src_ref=mine, dst_ref=mine, send_sem=wh_sem.at[0], recv_sem=wh_sem.at[1],
        device_id={"tile": sibling}, device_id_type=MESH,
    )
    swap.start()
    for strip_off in ready[done:]:
        near_step(strip_off)
    swap.wait_recv()

    for j in range(TILES // 2):
        strip = 2 * j + core
        extra = whole[ranks[strip]]
        total = near[j] + jnp.where(marks[0, strip] > 0, extra, 0.0)
        osend[j] = side_by_side(total)
    outs = [exchange(off, osend, mixed.at[chip], o_ssem, o_rsem) for off in ORDER]
    mixed[chip] = osend[chip]
    load_o.wait()

    def project_heads(heads):
        total = None
        for head in heads:
            block = jnp.concatenate(stacked(mixed[head]), axis=0).T
            part = jnp.dot(block.astype(BF16), wo[head], preferred_element_type=F32)
            total = part if total is None else total + part
        return total

    for copy in outs[:EARLY]:
        copy.wait_recv()
    branch[...] = project_heads([chip] + [pair_of(off) for off in ORDER[:EARLY]])
    for copy in outs[EARLY:]:
        copy.wait_recv()
    result = branch[...] + project_heads([pair_of(off) for off in ORDER[EARLY:]])
    out_ref[...] = (x_ref[...].astype(F32) + mod_row(2) * result).astype(BF16)

    for copy in mod_copies + q_passed + kv_sent + kv_passed + outs + [swap]:
        copy.wait_send()


def on_device(latents, condition, w_modulate, w_project, w_output, detail):
    hbm = pl.BlockSpec(memory_space=pl.ANY)
    dma = pltpu.SemaphoreType.DMA
    updated = pl.pallas_call(
        body,
        out_shape=pltpu.VMEM((STRIP, D), BF16),
        in_specs=[hbm] * 6,
        out_specs=pl.BlockSpec(memory_space=pltpu.VMEM),
        scratch_shapes=[
            pltpu.VMEM((STRIP, D), BF16),
            pltpu.VMEM((GROUPS, D), BF16),
            pltpu.VMEM((COLS, D), BF16),
            pltpu.VMEM((3, D, D), BF16),
            pltpu.VMEM((HEADS, HEAD, D), BF16),
            pltpu.VMEM((GROUPS, SPAN), F32),
            pltpu.VMEM((GROUPS, 8, 128), F32),
            pltpu.VMEM((GROUPS - 1, 8, 128), F32),
            pltpu.VMEM((32, 128), F32),
            pltpu.VMEM((3, D, STRIP), F32),
            pltpu.VMEM((HEADS, 8, D), BF16),
            pltpu.VMEM((HEADS, 2 * HEAD, STRIP), BF16),
            pltpu.VMEM((TILES, 8, D), BF16),
            pltpu.VMEM((TILES, 2 * HEAD, STRIP), BF16),
            pltpu.VMEM(((TILES + 2) * STRIP, PAD), BF16),
            pltpu.VMEM((PAD, WIDE), BF16),
            pltpu.VMEM((2, 2 * STRIP, WIDE), F32),
            pltpu.VMEM((TILES // 2, HEAD, STRIP), F32),
            pltpu.VMEM((SLOTS, HEAD, STRIP), F32),
            pltpu.VMEM((STRIP, D), F32),
            pltpu.VMEM((HEADS, 8, D), BF16),
            pltpu.VMEM((HEADS, 8, D), BF16),
            pltpu.SMEM((1, TILES), jnp.int32),
            pltpu.SMEM((TILES,), jnp.int32),
            dma((11,)),
            dma((GROUPS - 1,)), dma((GROUPS - 1,)),
            dma((HEADS,)), dma((HEADS,)),
            dma((HEADS,)), dma((HEADS,)),
            dma((HEADS,)), dma((HEADS,)),
            dma((HEADS,)), dma((HEADS,)),
            dma((2,)),
            dma((HEADS,)), dma((HEADS,)),
            pltpu.SemaphoreType.REGULAR((4,)),
        ],
        compiler_params=pltpu.CompilerParams(
            collective_id=0, has_side_effects=True, vmem_limit_bytes=56 * 1024 * 1024
        ),
    )(latents[0], condition, w_modulate.T, w_project, w_output.reshape(HEADS, HEAD, D), detail)
    return updated[None]


def solution(mesh):
    in_specs = (P("grp", "tile", None), P(), P(None, "grp"), P(), P(), P("grp", None))
    out_specs = P("grp", "tile", None)
    return jax.shard_map(
        on_device, mesh=mesh, in_specs=in_specs, out_specs=out_specs, check_vma=False
    )
```

```python
import functools

import jax
import jax.numpy as jnp
from jax import lax
from jax.experimental import pallas as pl
from jax.experimental.pallas import tpu as pltpu
from jax.sharding import PartitionSpec as P

HEADS = 16
HEAD = 72
D = HEADS * HEAD
STRIP = 128
MARGIN = 64
TILES = 32
SLOTS = 8
GROUPS = 8
COLS = 3 * D // GROUPS
SPAN = 640
PAD = 80
V_AT = HEAD - 8
SIDE = SLOTS // 2
WIDE = SIDE * STRIP
TILE_ROWS = 5
AHEAD = 2
EARLY = 9
EXP_SCALE = 1.4426950408889634 / (HEAD ** 0.5)
MESH = pl.DeviceIdType.MESH
F32 = jnp.float32
BF16 = jnp.bfloat16
ORDER = (1, 15, 3, 14, 2, 5, 13, 4, 12, 11, 7, 10, 6, 9, 8)
PARTS = (0, 128, 256, COLS)


def side_by_side(block):
    return jnp.concatenate([block[8 * r : 8 * r + 8] for r in range(HEAD // 8)], axis=1).astype(BF16)


def stacked(message):
    block = message.astype(F32)
    return [block[:, 128 * r : 128 * r + 128] for r in range(HEAD // 8)]


def queries(message):
    return jnp.concatenate(stacked(message) + [jnp.zeros((PAD - HEAD, STRIP), F32)], axis=0).astype(BF16)


def body(
    x_hbm, cond_hbm, wm_hbm, wp_hbm, wo_hbm, marks_hbm,
    out_ref,
    x_ref, cond, wm, wp, wo, mod_cols, mod_send, mod_recv, mod, proj, qsend, kvsend, qbuf, kvbuf, keys, q4,
    score_buf, near, whole, branch, osend, mixed, marks, ranks,
    load_sem, mod_ssem, mod_rsem, q_ssem, q_rsem, kv_ssem, kv_rsem, qf_ssem, qf_rsem, kvf_ssem, kvf_rsem,
    wh_sem, o_ssem, o_rsem, rounds,
):
    me = lax.axis_index("tile")
    grp = lax.axis_index("grp")
    chip = me // 2
    core = me % 2
    sibling = me + 1 - 2 * core

    barrier = pltpu.get_barrier_semaphore()
    across = me + 2 - 4 * (chip % 2)
    around = [[(me + far) % TILES, (me + TILES - far) % TILES] for far in (8, 4)]
    near_peers = around[0] + around[1] + [across, (across + 4) % TILES, (across + TILES - 4) % TILES, sibling]
    for near_by in near_peers:
        pl.semaphore_signal(barrier, inc=1, device_id={"tile": near_by}, device_id_type=MESH)
    for off in range(1, GROUPS):
        pl.semaphore_signal(barrier, inc=1, device_id={"grp": (grp + off) % GROUPS}, device_id_type=MESH)

    def tell(step):
        for near_by in around[step]:
            pl.semaphore_signal(rounds.at[step], inc=1, device_id={"tile": near_by}, device_id_type=MESH)

    def hear(step):
        pl.semaphore_wait(rounds.at[step], 2)

    load_c = pltpu.make_async_copy(cond_hbm, cond, load_sem.at[6])
    load_m = [
        pltpu.make_async_copy(wm_hbm.at[pl.ds(a, b - a)], wm.at[pl.ds(a, b - a)], load_sem.at[8 + i])
        for i, (a, b) in enumerate(zip(PARTS, PARTS[1:]))
    ]
    load_x = pltpu.make_async_copy(x_hbm, x_ref, load_sem.at[1])
    load_d = pltpu.make_async_copy(marks_hbm, marks, load_sem.at[7])
    load_p = [
        pltpu.make_async_copy(wp_hbm.at[:, pl.ds(D * i, D)], wp.at[i], load_sem.at[2 + i]) for i in range(3)
    ]
    load_o = pltpu.make_async_copy(wo_hbm, wo, load_sem.at[5])
    for copy in [load_c] + load_m + [load_x, load_d]:
        copy.start()

    mod_cols[...] = jnp.zeros_like(mod_cols)
    mod_send[...] = jnp.zeros_like(mod_send)
    mod[...] = jnp.zeros_like(mod)
    load_c.wait()
    for copy in load_m:
        copy.wait()
    for copy in load_p + [load_o]:
        copy.start()
    mod_cols[:, :COLS] = lax.dot_general(
        cond[...], wm[...], (((1,), (1,)), ((), ())), preferred_element_type=F32
    )
    shifted = pltpu.roll(mod_cols[...], (grp * COLS) % 128, axis=1)
    for i in range(TILE_ROWS):
        mod_send[:, i, :] = shifted[:, i * 128 : (i + 1) * 128]

    pl.semaphore_wait(barrier, GROUPS - 1 + len(near_peers))

    mod_copies = []
    for off in range(1, GROUPS):
        image = (grp + off) % GROUPS
        copy = pltpu.make_async_remote_copy(
            src_ref=mod_send.at[image], dst_ref=mod_recv.at[off - 1],
            send_sem=mod_ssem.at[off - 1], recv_sem=mod_rsem.at[off - 1],
            device_id={"grp": image}, device_id_type=MESH,
        )
        copy.start()
        mod_copies.append(copy)

    tell(0)
    load_x.wait()
    values32 = x_ref[...].astype(F32)
    mean = jnp.mean(values32, axis=1, keepdims=True)
    centered = values32 - mean
    variance = jnp.mean(centered * centered, axis=1, keepdims=True)
    unit = centered / jnp.sqrt(variance + 1e-06)

    hear(0)
    tell(1)

    load_d.wait()
    rank = jnp.int32(0)
    slots = [jnp.int32(0)] * SIDE
    for t in range(TILES):
        mark = marks[0, t]
        for j in range(SIDE):
            hit = jnp.logical_and(mark > 0, rank == core * SIDE + j)
            slots[j] = jnp.where(hit, jnp.int32(t), slots[j])
        ranks[t] = jnp.minimum(rank, SLOTS - 1)
        rank = rank + mark

    def add_columns(source, block):
        rows = pl.ds((source * COLS) // 128, TILE_ROWS)
        mod[rows, :] += block[0:TILE_ROWS]

    add_columns(grp, mod_send[grp])
    for off in range(1, GROUPS):
        mod_copies[off - 1].wait_recv()
        add_columns((grp + GROUPS - off) % GROUPS, mod_recv[off - 1])

    def mod_row(part):
        first = part * D // 128
        return jnp.concatenate([mod[first + i : first + i + 1, :] for i in range(D // 128)], axis=1)

    normed = (unit * (1.0 + mod_row(1)) + mod_row(0)).astype(BF16)

    def project(part):
        load_p[part].wait()
        proj[part] = jnp.dot(normed, wp[part], preferred_element_type=F32).T

    def exchange(off, src, dst, ssem, rsem):
        other = (chip + off) % HEADS
        copy = pltpu.make_async_remote_copy(
            src_ref=src.at[other], dst_ref=dst, send_sem=ssem.at[off], recv_sem=rsem.at[off],
            device_id={"tile": other * 2 + core}, device_id_type=MESH,
        )
        copy.start()
        return copy

    def forward(off, src, dst, ssem, rsem):
        copy = pltpu.make_async_remote_copy(
            src_ref=src, dst_ref=dst.at[strip_of(off, core)], send_sem=ssem.at[off], recv_sem=rsem.at[off],
            device_id={"tile": sibling}, device_id_type=MESH,
        )
        copy.start()
        return copy

    def strip_of(off, parity):
        return ((chip + HEADS - off) % HEADS) * 2 + parity

    project(0)
    for h in range(HEADS):
        qsend[h] = side_by_side(proj[0, h * HEAD : (h + 1) * HEAD, :])
    hear(1)
    q_sent = [exchange(off, qsend, qbuf.at[me], q_ssem, q_rsem) for off in ORDER]
    q_passed = [forward(0, qsend.at[chip], qbuf, qf_ssem, qf_rsem)]
    qbuf[me] = qsend[chip]
    project(1)
    project(2)
    for h in range(HEADS):
        rows = slice(h * HEAD, (h + 1) * HEAD)
        kvsend[h] = jnp.concatenate([proj[1, rows, :], proj[2, rows, :]], axis=0).astype(BF16)
    kv_sent = []
    kv_passed = [forward(0, kvsend.at[chip], kvbuf, kvf_ssem, kvf_rsem)]
    kvbuf[me] = kvsend[chip]
    keys[pl.ds(0, STRIP), :] = jnp.zeros((STRIP, PAD), BF16)
    keys[pl.ds((TILES + 1) * STRIP, STRIP), :] = jnp.zeros((STRIP, PAD), BF16)

    for off, copy in zip(ORDER, q_sent):
        copy.wait_send()
        kv_sent.append(exchange(off, kvsend, kvbuf.at[me], kv_ssem, kv_rsem))
    for off, copy in zip(ORDER, q_sent):
        copy.wait_recv()
        q_passed.append(forward(off, qbuf.at[strip_of(off, core)], qbuf, qf_ssem, qf_rsem))
    for copy in q_passed:
        copy.wait_recv()
    for j in range(SIDE):
        q4[:, j * STRIP : (j + 1) * STRIP] = queries(qbuf[slots[j]])

    def pair_of(off):
        return (chip + HEADS - off) % HEADS

    def scores_step(i, off, top):
        pair = pair_of(off)
        for parity in range(2):
            strip = pair * 2 + parity
            block = kvbuf[strip, 0:PAD, :].astype(F32).T
            keys[pl.ds(pl.multiple_of((strip + 1) * STRIP, STRIP), STRIP), :] = block.astype(BF16)
        block = keys[pl.ds(pl.multiple_of((2 * pair + 1) * STRIP, STRIP), 2 * STRIP), :]
        scores = jnp.dot(block, q4[...], preferred_element_type=F32)
        score_buf[i % 2] = scores
        return jnp.maximum(top, jnp.max(scores, axis=0, keepdims=True))

    def values_step(i, off, before, top, total, acc):
        pair = pair_of(off)
        factor = jnp.exp2((before - top) * EXP_SCALE)
        probs = jnp.exp2((score_buf[i % 2] - top) * EXP_SCALE)
        total = total * factor + jnp.sum(probs, axis=0, keepdims=True)
        rows = slice(V_AT, V_AT + PAD)
        values = jnp.concatenate([kvbuf[2 * pair, rows, :], kvbuf[2 * pair + 1, rows, :]], axis=1)
        acc = acc * factor + jnp.dot(values, probs.astype(BF16), preferred_element_type=F32)
        return total, acc

    def near_step(off):
        pair = pair_of(off)
        strip = 2 * pair + core
        block = keys[pl.ds(pl.multiple_of((strip + 1) * STRIP - MARGIN, MARGIN), 2 * STRIP), :]
        scores = jnp.dot(block, queries(qbuf[strip]), preferred_element_type=F32)
        at = strip * STRIP - MARGIN + lax.broadcasted_iota(jnp.int32, scores.shape, 0)
        scores = jnp.where(jnp.logical_and(at >= 0, at < TILES * STRIP), scores, -1e30)
        probs = jnp.exp2((scores - jnp.max(scores, axis=0, keepdims=True)) * EXP_SCALE)
        sums = jnp.sum(probs, axis=0, keepdims=True)
        blank = jnp.zeros((MARGIN, STRIP), BF16)
        weights = jnp.concatenate([blank, probs.astype(BF16), blank], axis=0)
        rows = pl.ds(V_AT, PAD)
        values = jnp.concatenate(
            [
                kvbuf[jnp.maximum(strip - 1, 0), rows, :],
                kvbuf[strip, rows, :],
                kvbuf[jnp.minimum(strip + 1, TILES - 1), rows, :],
            ],
            axis=1,
        )
        near[pair] = (jnp.dot(values, weights, preferred_element_type=F32) / sums)[8:PAD]

    steps = (0,) + ORDER
    total = jnp.zeros((1, WIDE), F32)
    acc = jnp.zeros((PAD, WIDE), F32)
    tops = [jnp.full((1, WIDE), -1e30, F32)]
    ready = []
    done = 0
    for i, off in enumerate(steps):
        while len(kv_passed) < min(i + AHEAD + 1, len(steps)):
            kv_sent[len(kv_passed) - 1].wait_recv()
            later = steps[len(kv_passed)]
            kv_passed.append(forward(later, kvbuf.at[strip_of(later, core)], kvbuf, kvf_ssem, kvf_rsem))
        kv_passed[i].wait_recv()
        tops.append(scores_step(i, off, tops[i]))
        if i > 0:
            total, acc = values_step(i - 1, steps[i - 1], tops[i - 1], tops[i], total, acc)
            if i + 1 < len(steps):
                for strip_off in ready[done:]:
                    near_step(strip_off)
                done = len(ready)
        come = steps[: i + 1]
        for o in come:
            if o not in ready and (o + 1) % HEADS in come and (o - 1) % HEADS in come:
                ready.append(o)
    last = len(steps) - 1
    total, acc = values_step(last, steps[last], tops[last], tops[last + 1], total, acc)
    result = acc / total
    for j in range(SIDE):
        whole[core * SIDE + j] = result[8:PAD, j * STRIP : (j + 1) * STRIP]
    mine = whole.at[pl.ds(core * SIDE, SIDE)]
    swap = pltpu.make_async_remote_copy(
        src_ref=mine, dst_ref=mine, send_sem=wh_sem.at[0], recv_sem=wh_sem.at[1],
        device_id={"tile": sibling}, device_id_type=MESH,
    )
    swap.start()
    for strip_off in ready[done:]:
        near_step(strip_off)
    swap.wait_recv()

    for j in range(TILES // 2):
        strip = 2 * j + core
        extra = whole[ranks[strip]]
        total = near[j] + jnp.where(marks[0, strip] > 0, extra, 0.0)
        osend[j] = side_by_side(total)
    outs = [exchange(off, osend, mixed.at[chip], o_ssem, o_rsem) for off in ORDER]
    mixed[chip] = osend[chip]
    load_o.wait()

    def project_heads(heads):
        total = None
        for head in heads:
            block = jnp.concatenate(stacked(mixed[head]), axis=0).T
            part = jnp.dot(block.astype(BF16), wo[head], preferred_element_type=F32)
            total = part if total is None else total + part
        return total

    for copy in outs[:EARLY]:
        copy.wait_recv()
    branch[...] = project_heads([chip] + [pair_of(off) for off in ORDER[:EARLY]])
    for copy in outs[EARLY:]:
        copy.wait_recv()
    result = branch[...] + project_heads([pair_of(off) for off in ORDER[EARLY:]])
    out_ref[...] = (x_ref[...].astype(F32) + mod_row(2) * result).astype(BF16)

    for copy in mod_copies + q_passed + kv_sent + kv_passed + outs + [swap]:
        copy.wait_send()


def on_device(latents, condition, w_modulate, w_project, w_output, detail):
    hbm = pl.BlockSpec(memory_space=pl.ANY)
    dma = pltpu.SemaphoreType.DMA
    updated = pl.pallas_call(
        body,
        out_shape=pltpu.VMEM((STRIP, D), BF16),
        in_specs=[hbm] * 6,
        out_specs=pl.BlockSpec(memory_space=pltpu.VMEM),
        scratch_shapes=[
            pltpu.VMEM((STRIP, D), BF16),
            pltpu.VMEM((GROUPS, D), BF16),
            pltpu.VMEM((COLS, D), BF16),
            pltpu.VMEM((3, D, D), BF16),
            pltpu.VMEM((HEADS, HEAD, D), BF16),
            pltpu.VMEM((GROUPS, SPAN), F32),
            pltpu.VMEM((GROUPS, 8, 128), F32),
            pltpu.VMEM((GROUPS - 1, 8, 128), F32),
            pltpu.VMEM((32, 128), F32),
            pltpu.VMEM((3, D, STRIP), F32),
            pltpu.VMEM((HEADS, 8, D), BF16),
            pltpu.VMEM((HEADS, 2 * HEAD, STRIP), BF16),
            pltpu.VMEM((TILES, 8, D), BF16),
            pltpu.VMEM((TILES, 2 * HEAD, STRIP), BF16),
            pltpu.VMEM(((TILES + 2) * STRIP, PAD), BF16),
            pltpu.VMEM((PAD, WIDE), BF16),
            pltpu.VMEM((2, 2 * STRIP, WIDE), F32),
            pltpu.VMEM((TILES // 2, HEAD, STRIP), F32),
            pltpu.VMEM((SLOTS, HEAD, STRIP), F32),
            pltpu.VMEM((STRIP, D), F32),
            pltpu.VMEM((HEADS, 8, D), BF16),
            pltpu.VMEM((HEADS, 8, D), BF16),
            pltpu.SMEM((1, TILES), jnp.int32),
            pltpu.SMEM((TILES,), jnp.int32),
            dma((11,)),
            dma((GROUPS - 1,)), dma((GROUPS - 1,)),
            dma((HEADS,)), dma((HEADS,)),
            dma((HEADS,)), dma((HEADS,)),
            dma((HEADS,)), dma((HEADS,)),
            dma((HEADS,)), dma((HEADS,)),
            dma((2,)),
            dma((HEADS,)), dma((HEADS,)),
            pltpu.SemaphoreType.REGULAR((2,)),
        ],
        compiler_params=pltpu.CompilerParams(
            collective_id=0, has_side_effects=True, vmem_limit_bytes=56 * 1024 * 1024
        ),
    )(latents[0], condition, w_modulate.T, w_project, w_output.reshape(HEADS, HEAD, D), detail)
    return updated[None]


def solution(mesh):
    in_specs = (P("grp", "tile", None), P(), P(None, "grp"), P(), P(), P("grp", None))
    out_specs = P("grp", "tile", None)
    return jax.shard_map(
        on_device, mesh=mesh, in_specs=in_specs, out_specs=out_specs, check_vma=False
    )
```

```python
import functools

import jax
import jax.numpy as jnp
from jax import lax
from jax.experimental import pallas as pl
from jax.experimental.pallas import tpu as pltpu
from jax.sharding import PartitionSpec as P

HEADS = 16
HEAD = 72
D = HEADS * HEAD
STRIP = 128
MARGIN = 64
TILES = 32
SLOTS = 8
GROUPS = 8
COLS = 3 * D // GROUPS
SPAN = 640
PAD = 80
V_AT = HEAD - 8
SIDE = SLOTS // 2
WIDE = SIDE * STRIP
TILE_ROWS = 5
AHEAD = 2
EXP_SCALE = 1.4426950408889634 / (HEAD ** 0.5)
MESH = pl.DeviceIdType.MESH
F32 = jnp.float32
BF16 = jnp.bfloat16
ORDER = (1, 15, 3, 14, 2, 5, 13, 4, 12, 11, 7, 10, 6, 9, 8)
PARTS = (0, 128, 256, COLS)


def side_by_side(block):
    return jnp.concatenate([block[8 * r : 8 * r + 8] for r in range(HEAD // 8)], axis=1).astype(BF16)


def stacked(message):
    block = message.astype(F32)
    return [block[:, 128 * r : 128 * r + 128] for r in range(HEAD // 8)]


def queries(message):
    return jnp.concatenate(stacked(message) + [jnp.zeros((PAD - HEAD, STRIP), F32)], axis=0).astype(BF16)


def body(
    x_hbm, cond_hbm, wm_hbm, wp_hbm, wo_hbm, marks_hbm,
    out_ref,
    x_ref, cond, wm, wp, wo, mod_cols, mod_send, mod_recv, mod, proj, qsend, kvsend, qbuf, kvbuf, keys, q4,
    score_buf, near, whole, osend, mixed, marks, ranks,
    load_sem, mod_ssem, mod_rsem, q_ssem, q_rsem, kv_ssem, kv_rsem, qf_ssem, qf_rsem, kvf_ssem, kvf_rsem,
    wh_sem, o_ssem, o_rsem, rounds,
):
    me = lax.axis_index("tile")
    grp = lax.axis_index("grp")
    chip = me // 2
    core = me % 2
    sibling = me + 1 - 2 * core

    barrier = pltpu.get_barrier_semaphore()
    across = me + 2 - 4 * (chip % 2)
    around = [[(me + far) % TILES, (me + TILES - far) % TILES] for far in (8, 4)]
    near_peers = around[0] + around[1] + [across, (across + 4) % TILES, (across + TILES - 4) % TILES, sibling]
    for near_by in near_peers:
        pl.semaphore_signal(barrier, inc=1, device_id={"tile": near_by}, device_id_type=MESH)
    for off in range(1, GROUPS):
        pl.semaphore_signal(barrier, inc=1, device_id={"grp": (grp + off) % GROUPS}, device_id_type=MESH)

    def tell(step):
        for near_by in around[step]:
            pl.semaphore_signal(rounds.at[step], inc=1, device_id={"tile": near_by}, device_id_type=MESH)

    def hear(step):
        pl.semaphore_wait(rounds.at[step], 2)

    load_c = pltpu.make_async_copy(cond_hbm, cond, load_sem.at[6])
    load_m = [
        pltpu.make_async_copy(wm_hbm.at[pl.ds(a, b - a)], wm.at[pl.ds(a, b - a)], load_sem.at[8 + i])
        for i, (a, b) in enumerate(zip(PARTS, PARTS[1:]))
    ]
    load_x = pltpu.make_async_copy(x_hbm, x_ref, load_sem.at[1])
    load_d = pltpu.make_async_copy(marks_hbm, marks, load_sem.at[7])
    load_p = [
        pltpu.make_async_copy(wp_hbm.at[:, pl.ds(D * i, D)], wp.at[i], load_sem.at[2 + i]) for i in range(3)
    ]
    load_o = pltpu.make_async_copy(wo_hbm, wo, load_sem.at[5])
    for copy in [load_c] + load_m + [load_x, load_d]:
        copy.start()

    mod_cols[...] = jnp.zeros_like(mod_cols)
    mod_send[...] = jnp.zeros_like(mod_send)
    mod[...] = jnp.zeros_like(mod)
    load_c.wait()
    for copy in load_m:
        copy.wait()
    for copy in load_p + [load_o]:
        copy.start()
    mod_cols[:, :COLS] = lax.dot_general(
        cond[...], wm[...], (((1,), (1,)), ((), ())), preferred_element_type=F32
    )
    shifted = pltpu.roll(mod_cols[...], (grp * COLS) % 128, axis=1)
    for i in range(TILE_ROWS):
        mod_send[:, i, :] = shifted[:, i * 128 : (i + 1) * 128]

    pl.semaphore_wait(barrier, GROUPS - 1 + len(near_peers))

    mod_copies = []
    for off in range(1, GROUPS):
        image = (grp + off) % GROUPS
        copy = pltpu.make_async_remote_copy(
            src_ref=mod_send.at[image], dst_ref=mod_recv.at[off - 1],
            send_sem=mod_ssem.at[off - 1], recv_sem=mod_rsem.at[off - 1],
            device_id={"grp": image}, device_id_type=MESH,
        )
        copy.start()
        mod_copies.append(copy)

    tell(0)
    load_x.wait()
    values32 = x_ref[...].astype(F32)
    mean = jnp.mean(values32, axis=1, keepdims=True)
    centered = values32 - mean
    variance = jnp.mean(centered * centered, axis=1, keepdims=True)
    unit = centered / jnp.sqrt(variance + 1e-06)

    hear(0)
    tell(1)

    load_d.wait()
    rank = jnp.int32(0)
    slots = [jnp.int32(0)] * SIDE
    for t in range(TILES):
        mark = marks[0, t]
        for j in range(SIDE):
            hit = jnp.logical_and(mark > 0, rank == core * SIDE + j)
            slots[j] = jnp.where(hit, jnp.int32(t), slots[j])
        ranks[t] = jnp.minimum(rank, SLOTS - 1)
        rank = rank + mark

    def add_columns(source, block):
        rows = pl.ds((source * COLS) // 128, TILE_ROWS)
        mod[rows, :] += block[0:TILE_ROWS]

    add_columns(grp, mod_send[grp])
    for off in range(1, GROUPS):
        mod_copies[off - 1].wait_recv()
        add_columns((grp + GROUPS - off) % GROUPS, mod_recv[off - 1])

    def mod_row(part):
        first = part * D // 128
        return jnp.concatenate([mod[first + i : first + i + 1, :] for i in range(D // 128)], axis=1)

    normed = (unit * (1.0 + mod_row(1)) + mod_row(0)).astype(BF16)

    def project(part):
        load_p[part].wait()
        proj[part] = jnp.dot(normed, wp[part], preferred_element_type=F32).T

    def exchange(off, src, dst, ssem, rsem):
        other = (chip + off) % HEADS
        copy = pltpu.make_async_remote_copy(
            src_ref=src.at[other], dst_ref=dst, send_sem=ssem.at[off], recv_sem=rsem.at[off],
            device_id={"tile": other * 2 + core}, device_id_type=MESH,
        )
        copy.start()
        return copy

    def forward(off, src, dst, ssem, rsem):
        copy = pltpu.make_async_remote_copy(
            src_ref=src, dst_ref=dst.at[strip_of(off, core)], send_sem=ssem.at[off], recv_sem=rsem.at[off],
            device_id={"tile": sibling}, device_id_type=MESH,
        )
        copy.start()
        return copy

    def strip_of(off, parity):
        return ((chip + HEADS - off) % HEADS) * 2 + parity

    project(0)
    for h in range(HEADS):
        qsend[h] = side_by_side(proj[0, h * HEAD : (h + 1) * HEAD, :])
    hear(1)
    q_sent = [exchange(off, qsend, qbuf.at[me], q_ssem, q_rsem) for off in ORDER]
    q_passed = [forward(0, qsend.at[chip], qbuf, qf_ssem, qf_rsem)]
    qbuf[me] = qsend[chip]
    project(1)
    project(2)
    for h in range(HEADS):
        rows = slice(h * HEAD, (h + 1) * HEAD)
        kvsend[h] = jnp.concatenate([proj[1, rows, :], proj[2, rows, :]], axis=0).astype(BF16)
    kv_sent = []
    kv_passed = [forward(0, kvsend.at[chip], kvbuf, kvf_ssem, kvf_rsem)]
    kvbuf[me] = kvsend[chip]
    keys[pl.ds(0, STRIP), :] = jnp.zeros((STRIP, PAD), BF16)
    keys[pl.ds((TILES + 1) * STRIP, STRIP), :] = jnp.zeros((STRIP, PAD), BF16)

    for off, copy in zip(ORDER, q_sent):
        copy.wait_send()
        kv_sent.append(exchange(off, kvsend, kvbuf.at[me], kv_ssem, kv_rsem))
    for off, copy in zip(ORDER, q_sent):
        copy.wait_recv()
        q_passed.append(forward(off, qbuf.at[strip_of(off, core)], qbuf, qf_ssem, qf_rsem))
    for copy in q_passed:
        copy.wait_recv()
    for j in range(SIDE):
        q4[:, j * STRIP : (j + 1) * STRIP] = queries(qbuf[slots[j]])

    def pair_of(off):
        return (chip + HEADS - off) % HEADS

    def scores_step(i, off, top):
        pair = pair_of(off)
        for parity in range(2):
            strip = pair * 2 + parity
            block = kvbuf[strip, 0:PAD, :].astype(F32).T
            keys[pl.ds(pl.multiple_of((strip + 1) * STRIP, STRIP), STRIP), :] = block.astype(BF16)
        block = keys[pl.ds(pl.multiple_of((2 * pair + 1) * STRIP, STRIP), 2 * STRIP), :]
        scores = jnp.dot(block, q4[...], preferred_element_type=F32)
        score_buf[i % 2] = scores
        return jnp.maximum(top, jnp.max(scores, axis=0, keepdims=True))

    def values_step(i, off, before, top, total, acc):
        pair = pair_of(off)
        factor = jnp.exp2((before - top) * EXP_SCALE)
        probs = jnp.exp2((score_buf[i % 2] - top) * EXP_SCALE)
        total = total * factor + jnp.sum(probs, axis=0, keepdims=True)
        rows = slice(V_AT, V_AT + PAD)
        values = jnp.concatenate([kvbuf[2 * pair, rows, :], kvbuf[2 * pair + 1, rows, :]], axis=1)
        acc = acc * factor + jnp.dot(values, probs.astype(BF16), preferred_element_type=F32)
        return total, acc

    def near_step(off):
        pair = pair_of(off)
        strip = 2 * pair + core
        block = keys[pl.ds(pl.multiple_of((strip + 1) * STRIP - MARGIN, MARGIN), 2 * STRIP), :]
        scores = jnp.dot(block, queries(qbuf[strip]), preferred_element_type=F32)
        at = strip * STRIP - MARGIN + lax.broadcasted_iota(jnp.int32, scores.shape, 0)
        scores = jnp.where(jnp.logical_and(at >= 0, at < TILES * STRIP), scores, -1e30)
        probs = jnp.exp2((scores - jnp.max(scores, axis=0, keepdims=True)) * EXP_SCALE)
        sums = jnp.sum(probs, axis=0, keepdims=True)
        blank = jnp.zeros((MARGIN, STRIP), BF16)
        weights = jnp.concatenate([blank, probs.astype(BF16), blank], axis=0)
        rows = pl.ds(V_AT, PAD)
        values = jnp.concatenate(
            [
                kvbuf[jnp.maximum(strip - 1, 0), rows, :],
                kvbuf[strip, rows, :],
                kvbuf[jnp.minimum(strip + 1, TILES - 1), rows, :],
            ],
            axis=1,
        )
        near[pair] = (jnp.dot(values, weights, preferred_element_type=F32) / sums)[8:PAD]

    steps = (0,) + ORDER
    total = jnp.zeros((1, WIDE), F32)
    acc = jnp.zeros((PAD, WIDE), F32)
    tops = [jnp.full((1, WIDE), -1e30, F32)]
    ready = []
    done = 0
    for i, off in enumerate(steps):
        while len(kv_passed) < min(i + AHEAD + 1, len(steps)):
            kv_sent[len(kv_passed) - 1].wait_recv()
            later = steps[len(kv_passed)]
            kv_passed.append(forward(later, kvbuf.at[strip_of(later, core)], kvbuf, kvf_ssem, kvf_rsem))
        kv_passed[i].wait_recv()
        tops.append(scores_step(i, off, tops[i]))
        if i > 0:
            total, acc = values_step(i - 1, steps[i - 1], tops[i - 1], tops[i], total, acc)
            if i + 1 < len(steps):
                for strip_off in ready[done:]:
                    near_step(strip_off)
                done = len(ready)
        come = steps[: i + 1]
        for o in come:
            if o not in ready and (o + 1) % HEADS in come and (o - 1) % HEADS in come:
                ready.append(o)
    last = len(steps) - 1
    total, acc = values_step(last, steps[last], tops[last], tops[last + 1], total, acc)
    result = acc / total
    for j in range(SIDE):
        whole[core * SIDE + j] = result[8:PAD, j * STRIP : (j + 1) * STRIP]
    mine = whole.at[pl.ds(core * SIDE, SIDE)]
    swap = pltpu.make_async_remote_copy(
        src_ref=mine, dst_ref=mine, send_sem=wh_sem.at[0], recv_sem=wh_sem.at[1],
        device_id={"tile": sibling}, device_id_type=MESH,
    )
    swap.start()
    for strip_off in ready[done:]:
        near_step(strip_off)
    swap.wait_recv()

    for j in range(TILES // 2):
        strip = 2 * j + core
        extra = whole[ranks[strip]]
        total = near[j] + jnp.where(marks[0, strip] > 0, extra, 0.0)
        osend[j] = side_by_side(total)
    outs = [exchange(off, osend, mixed.at[chip], o_ssem, o_rsem) for off in reversed(ORDER)]
    mixed[chip] = osend[chip]
    load_o.wait()

    for copy in outs:
        copy.wait_recv()
    gathered = jnp.concatenate([row for h in range(HEADS) for row in stacked(mixed[h])], axis=0).T
    result = jnp.dot(gathered.astype(BF16), wo[...], preferred_element_type=F32)
    out_ref[...] = (x_ref[...].astype(F32) + mod_row(2) * result).astype(BF16)

    for copy in mod_copies + q_passed + kv_sent + kv_passed + outs + [swap]:
        copy.wait_send()


def on_device(latents, condition, w_modulate, w_project, w_output, detail):
    hbm = pl.BlockSpec(memory_space=pl.ANY)
    dma = pltpu.SemaphoreType.DMA
    updated = pl.pallas_call(
        body,
        out_shape=pltpu.VMEM((STRIP, D), BF16),
        in_specs=[hbm] * 6,
        out_specs=pl.BlockSpec(memory_space=pltpu.VMEM),
        scratch_shapes=[
            pltpu.VMEM((STRIP, D), BF16),
            pltpu.VMEM((GROUPS, D), BF16),
            pltpu.VMEM((COLS, D), BF16),
            pltpu.VMEM((3, D, D), BF16),
            pltpu.VMEM((D, D), BF16),
            pltpu.VMEM((GROUPS, SPAN), F32),
            pltpu.VMEM((GROUPS, 8, 128), F32),
            pltpu.VMEM((GROUPS - 1, 8, 128), F32),
            pltpu.VMEM((32, 128), F32),
            pltpu.VMEM((3, D, STRIP), F32),
            pltpu.VMEM((HEADS, 8, D), BF16),
            pltpu.VMEM((HEADS, 2 * HEAD, STRIP), BF16),
            pltpu.VMEM((TILES, 8, D), BF16),
            pltpu.VMEM((TILES, 2 * HEAD, STRIP), BF16),
            pltpu.VMEM(((TILES + 2) * STRIP, PAD), BF16),
            pltpu.VMEM((PAD, WIDE), BF16),
            pltpu.VMEM((2, 2 * STRIP, WIDE), F32),
            pltpu.VMEM((TILES // 2, HEAD, STRIP), F32),
            pltpu.VMEM((SLOTS, HEAD, STRIP), F32),
            pltpu.VMEM((HEADS, 8, D), BF16),
            pltpu.VMEM((HEADS, 8, D), BF16),
            pltpu.SMEM((1, TILES), jnp.int32),
            pltpu.SMEM((TILES,), jnp.int32),
            dma((11,)),
            dma((GROUPS - 1,)), dma((GROUPS - 1,)),
            dma((HEADS,)), dma((HEADS,)),
            dma((HEADS,)), dma((HEADS,)),
            dma((HEADS,)), dma((HEADS,)),
            dma((HEADS,)), dma((HEADS,)),
            dma((2,)),
            dma((HEADS,)), dma((HEADS,)),
            pltpu.SemaphoreType.REGULAR((2,)),
        ],
        compiler_params=pltpu.CompilerParams(
            collective_id=0, has_side_effects=True, vmem_limit_bytes=56 * 1024 * 1024
        ),
    )(latents[0], condition, w_modulate.T, w_project, w_output, detail)
    return updated[None]


def solution(mesh):
    in_specs = (P("grp", "tile", None), P(), P(None, "grp"), P(), P(), P("grp", None))
    out_specs = P("grp", "tile", None)
    return jax.shard_map(
        on_device, mesh=mesh, in_specs=in_specs, out_specs=out_specs, check_vma=False
    )
```
